32 devices in a mesh: rows: 4 (over x, core), cols: 8 (over z, y).
Axes of the slice: x: 2, y: 2, z: 4, core: 2. Of those that a mesh axis runs over, the one named last changes fastest.
Arguments:
- elevation: float32 [512, 8192], P('rows', 'cols'), may hold values from -6 to 6
- data_mask: int32 [512, 8192], P('rows', 'cols'), may hold values 0 or 1
- tie_order: int32 [8], replicated, may hold values from 0 to 7, each once
Outputs:
- inflow: float32 [512, 8192], P('rows', 'cols')
The draws below stay inside these ranges and needn't reach their ends.
Inputs may be any that keep to these rules, and one draw needn't show every extreme that they name: tie_order holds each of 0 to 7 once.
All inputs are finite; a program needn't handle non-finite values. No bound on the sum of `data_mask` on one device may be relied on, other than what follows from the above.
Results may differ from the reference program's by a relative error of at most 0.0003.
Values sent between devices are 32-bit elements; how exact they have to be, the bound alone decides.
A program may use at most 64 MiB of HBM per device.

```python
import jax
import jax.numpy as jnp
from jax import lax

TILE_COLUMNS = 1024
ITERS = 8
NR = 512
NC = 8192
N_COLS = 8


def plant(drawn, stream_key, low, high):
    spot = [jax.random.randint(jax.random.fold_in(stream_key, axis), (), 0, length) for axis, length in enumerate(drawn.shape)]
    widest = drawn.shape.index(max(drawn.shape))
    next_to = spot[:widest] + [(spot[widest] + 1) % drawn.shape[widest]] + spot[widest + 1:]
    return drawn.at[tuple(spot)].set(low).at[tuple(next_to)].set(high)


def block_levels(key, dims, shards, smallest, high):
    def one(axis_at, shards_of):
        heights = jax.random.uniform(jax.random.fold_in(jax.random.fold_in(key, 6), axis_at), (shards_of,), jnp.float32, smallest / len(shards), high / len(shards))
        return jnp.repeat(jnp.exp(heights), dims[axis_at] // shards_of).reshape((-1,) + (1,) * (len(dims) - axis_at - 1))

    level = one(*shards[0])
    for cut in shards[1:]:
        level = level * one(*cut)
    return level


def gaussian(key, shape, width, limit, shards=(), kind=jnp.bfloat16):
    drawn = jax.random.normal(key, shape, jnp.float32) * width
    if len(shards) > 0:
        drawn = block_levels(key, shape, shards, -0.22, 0.18) * drawn
    return jnp.clip(drawn, min=-limit, max=limit).astype(kind)


def setup_inputs(seed: int = 0) -> dict:
    key_list = jax.random.split(jax.random.key(seed), 4)
    return {
        "elevation": gaussian(key_list[0], (NR, NC), 1.0, 6.0, ((0, 4), (1, 8)), jnp.float32),
        "data_mask": plant((jax.random.randint(key_list[1], (NR, NC), 0, 4) < 3).astype(jnp.int32), jax.random.fold_in(key_list[1], 1), 0, 1),
        "tie_order": jax.random.permutation(key_list[2], 8).astype(jnp.int32),
    }


OFFSETS = ((0, 1), (1, 1), (1, 0), (1, -1), (0, -1), (-1, -1), (-1, 0), (-1, 1))
RECIPROCAL = (1.0, 0.7071067811865476, 1.0, 0.7071067811865476, 1.0, 0.7071067811865476, 1.0, 0.7071067811865476)
RETENTION = 0.1


def priorities(tie_order):
    places = jnp.arange(8, dtype=jnp.float32)
    values = 1.0 + 0.5 * (7.0 - places) / 7.0
    matches = (tie_order[:, None] == jnp.arange(8, dtype=jnp.int32)[None, :]).astype(jnp.float32)
    return jnp.sum(matches * values[:, None], axis=0)


def outflow_weight_matrix(height_pad, valid_pad, ranking_order):
    height = height_pad.shape[0] - 2
    breadth = height_pad.shape[1] - 2
    centre = height_pad[1:-1, 1:-1]
    slopes = []
    for number, (step_row, step_col) in enumerate(OFFSETS):
        beside = height_pad[1 + step_row:1 + step_row + height, 1 + step_col:1 + step_col + breadth]
        beside_ok = valid_pad[1 + step_row:1 + step_row + height, 1 + step_col:1 + step_col + breadth]
        slopes.append(beside_ok * ranking_order[number] * jnp.maximum(centre - beside, 0.0) * RECIPROCAL[number])
    slopes = jnp.stack(slopes)
    totals = jnp.sum(slopes, axis=0) + RETENTION
    return slopes / totals


def gather_inflow(weights, field_pad):
    height = field_pad.shape[0] - 2
    breadth = field_pad.shape[1] - 2
    summed_in = jnp.zeros((height, breadth), jnp.float32)
    for number, (step_row, step_col) in enumerate(OFFSETS):
        term = weights[number] * field_pad
        summed_in = summed_in + term[1 - step_row:1 - step_row + height, 1 - step_col:1 - step_col + breadth]
    return summed_in


def reference(elevation, data_mask, tie_order):
    ranking_order = priorities(tie_order)
    full_rows, full_cols = elevation.shape
    valid_flag = data_mask.astype(jnp.float32)
    over_rows, over_cols = full_rows // 8, full_cols // 8
    summed = (valid_flag * elevation).reshape(over_rows, 8, over_cols, 8).sum(axis=(1, 3))
    counts = valid_flag.reshape(over_rows, 8, over_cols, 8).sum(axis=(1, 3))
    overview = summed / (counts + 1.0)
    runoff = counts / 64.0
    coarse_w = outflow_weight_matrix(jnp.pad(overview, 2), jnp.pad(jnp.ones_like(overview), 2), ranking_order)
    flow_now = runoff
    for sweep in range(ITERS):
        flow_now = runoff + gather_inflow(coarse_w, jnp.pad(flow_now, 1))
    upsampled = jnp.repeat(jnp.repeat(flow_now, 8, axis=0), 8, axis=1)
    up_window = jnp.pad(upsampled, 1)
    elevation_window = jnp.pad(elevation, 2)
    valid_cols = jnp.pad(jnp.ones((full_cols,), jnp.float32), 2)
    valid_rows = jnp.pad(jnp.ones((full_rows,), jnp.float32), 2)

    def one_block(column_block):
        start_offset = (column_block * TILE_COLUMNS).astype(jnp.int32)
        height_values = lax.dynamic_slice_in_dim(elevation_window, start_offset, TILE_COLUMNS + 4, 1)
        valid_pad = valid_rows[:, None] * lax.dynamic_slice_in_dim(valid_cols, start_offset, TILE_COLUMNS + 4, 0)[None, :]
        ups = lax.dynamic_slice_in_dim(up_window, start_offset, TILE_COLUMNS + 2, 1)
        flags = lax.dynamic_slice_in_dim(valid_flag, start_offset, TILE_COLUMNS, 1)
        detailed_weight = outflow_weight_matrix(height_values, valid_pad, ranking_order)
        return flags + gather_inflow(detailed_weight, ups)

    blocks = lax.map(one_block, jnp.arange(N_COLS, dtype=jnp.int32))
    return jnp.moveaxis(blocks, 0, 1).reshape(full_rows, full_cols)
```

```python
import functools

import jax
import jax.numpy as jnp
from jax import lax
from jax.experimental import pallas as pl
from jax.experimental.pallas import tpu as pltpu
from jax.sharding import PartitionSpec as P

ITERS = 8
OFFSETS = ((0, 1), (1, 1), (1, 0), (1, -1), (0, -1), (-1, -1), (-1, 0), (-1, 1))
RECIPROCAL = (1.0, 0.7071067811865476) * 4
RETENTION = 0.1
OUTSIDE = 1000.0
LANES = 128
F32 = jnp.float32


def coefficients(tie_ref):
    out = []
    for k in range(8):
        value = jnp.float32(0.0)
        for i in range(8):
            place = jnp.float32((1.0 + 0.5 * (7.0 - i) / 7.0) * RECIPROCAL[k])
            value = jnp.where(tie_ref[i] == k, place, value)
        out.append(value)
    return out


def shift_lanes(before, here, after, step, lane):
    if step == 0:
        return here
    if step < 0:
        return pltpu.roll(jnp.where(lane == LANES - 1, before, here), 1, 1)
    return pltpu.roll(jnp.where(lane == 0, after, here), LANES - 1, 1)


def take_lanes(values, index):
    return jnp.take_along_axis(values, index, axis=1, mode="promise_in_bounds")


def kernel(row_devices, col_devices, tie_hbm, elev_ref, mask_ref, out_ref, tie_ref, zp, zl, zr, mask, recip, pending, base, inner, outer,
           inner_edge, outer_edge, turned, ones, side, tall, srecv, vrecv, load_sem, tie_sem, send_sem, recv_sem):
    rows, cols = elev_ref.shape
    groups, blocks = rows // 8, cols // LANES
    crows, halves = groups, groups // 8
    row, col = lax.axis_index("rows"), lax.axis_index("cols")
    far = blocks - 1

    loads = {}
    for j in [0, far] + list(range(1, far)):
        part = pl.ds(j * LANES, LANES)
        loads[j] = (
            pltpu.make_async_copy(elev_ref.at[:, part], zp.at[j, pl.ds(8, rows), :], load_sem.at[j]),
            pltpu.make_async_copy(mask_ref.at[:, part], mask.at[j], load_sem.at[blocks + j]))
        loads[j][0].start()
        loads[j][1].start()
    tie_load = pltpu.make_async_copy(tie_hbm, tie_ref, tie_sem)
    tie_load.start()

    barrier = pltpu.get_barrier_semaphore()
    exists = []
    for step_row, step_col in OFFSETS:
        there = jnp.bool_(True)
        if step_row > 0:
            there = row < row_devices - 1
        if step_row < 0:
            there = row > 0
        if step_col > 0:
            there = jnp.logical_and(there, col < col_devices - 1)
        if step_col < 0:
            there = jnp.logical_and(there, col > 0)
        exists.append(there)

    def peer(k):
        return {"rows": row + OFFSETS[k][0], "cols": col + OFFSETS[k][1]}

    for k in range(8):
        @pl.when(exists[k])
        def _():
            pl.semaphore_signal(barrier, inc=1, device_id=peer(k), device_id_type=pl.DeviceIdType.MESH)

    lane = lax.broadcasted_iota(jnp.int32, (8, LANES), 1)
    sub = lax.broadcasted_iota(jnp.int32, (8, LANES), 0)
    lane_c = lax.broadcasted_iota(jnp.int32, (crows, LANES), 1)
    middle_lanes = jnp.logical_and(lane_c >= LANES // 4, lane_c < 3 * LANES // 4)
    first, last = (lane & 7) == 0, (lane & 7) == 7
    half = LANES // 2
    nothing = jnp.zeros((8, LANES), F32)

    SIDES, UPDOWN = (0, 1, 3, 4, 5, 7), (2, 6)

    ones[...] = (
        lax.broadcasted_iota(jnp.int32, (cols, LANES), 0) // 8 == lax.broadcasted_iota(jnp.int32, (cols, LANES), 1)
    ).astype(F32).astype(jnp.bfloat16)

    loads[0][0].wait()
    loads[far][0].wait()
    ends = jnp.where(lax.broadcasted_iota(jnp.int32, (rows, LANES), 1) < half, zp[0, 8:8 + rows, :], zp[far, 8:8 + rows, :])
    ends = jnp.transpose(ends)
    tile = jnp.where(sub < 4, pltpu.roll(ends[0:8], 2, 0), pltpu.roll(ends[LANES - 8:LANES], 6, 0))
    side[crows:crows + 8, :] = tile
    tall[16 + 2 * crows:24 + 2 * crows, :] = tile

    total = jnp.zeros((4 * crows, LANES), F32)
    for j in loads:
        if j not in (0, far):
            loads[j][0].wait()
        loads[j][1].wait()
        height_sum = jnp.zeros((crows, LANES), F32)
        count_sum = jnp.zeros((crows, LANES), F32)
        for s in range(8):
            valid = mask[j, pl.ds(s, crows, stride=8), :].astype(F32)
            height_sum = height_sum + valid * zp[j, pl.ds(8 + s, crows, stride=8), :]
            count_sum = count_sum + valid
        high = height_sum.astype(jnp.bfloat16)
        rest = height_sum - high.astype(F32)
        middle = rest.astype(jnp.bfloat16)
        low = (rest - middle.astype(F32)).astype(jnp.bfloat16)
        stacked = jnp.concatenate([count_sum.astype(jnp.bfloat16), high, middle, low], axis=0)
        total = total + jnp.dot(stacked, ones[j * LANES:(j + 1) * LANES, :], preferred_element_type=F32)
        for number, at in enumerate((8, 9, rows + 6, rows + 7)):
            line = (0, 8, 24 + 2 * crows, 32 + 2 * crows)[number]
            tall[line + j:line + j + 1, :] = zp[j, at:at + 1, :]
    counts = total[0:crows]
    heights = total[crows:2 * crows] + (total[2 * crows:3 * crows] + total[3 * crows:])
    overview = heights / (counts + 1.0)
    runoff = counts * (1.0 / 64.0)
    side[0:crows, :] = jnp.where(middle_lanes, pltpu.roll(runoff, half, 1), overview)
    tall[16:16 + crows, :] = overview
    tall[16 + crows:16 + 2 * crows, :] = runoff

    pl.semaphore_wait(barrier, functools.reduce(jnp.add, [there.astype(jnp.int32) for there in exists]))

    def copies(k, arriving=False):
        slot = k if arriving else (k + 4) % 8
        if k in UPDOWN:
            src, dst = tall.at[pl.ds(16 if k == 2 else 0, 24 + 2 * crows), :], vrecv.at[slot // 4]
        else:
            src, dst = side, srecv.at[slot]
        return pltpu.make_async_remote_copy(
            src_ref=src, dst_ref=dst, send_sem=send_sem.at[k], recv_sem=recv_sem.at[slot],
            device_id=peer(k), device_id_type=pl.DeviceIdType.MESH)

    for k in (1, 3, 5, 7, 0, 4, 2, 6):
        @pl.when(exists[k])
        def _():
            copies(k).start()

    for k in range(8):
        @pl.when(jnp.logical_not(exists[k]))
        def _():
            if k in UPDOWN:
                for at in range(0, 24 + 2 * crows, 8):
                    start = 16 + crows if k == 2 else crows
                    vrecv[k // 4, at:at + 8, :] = jnp.full((8, LANES), 0.0 if start <= at < start + crows else OUTSIDE, F32)
            else:
                srecv[k, 0:crows, :] = jnp.where(middle_lanes, 0.0, OUTSIDE)
                srecv[k, crows:crows + 8, :] = jnp.full((8, LANES), OUTSIDE, F32)

    tie_load.wait()
    coef = coefficients(tie_ref)

    for g in range(groups):
        at = pl.ds(8 * g + 8, 8)
        for j in range(blocks):
            here = zp[j, at, :]
            before, after = zp[(j - 1) % blocks, at, :], zp[(j + 1) % blocks, at, :]
            zl[j, at, :] = shift_lanes(before, here, after, -1, lane)
            zr[j, at, :] = shift_lanes(before, here, after, 1, lane)
            base[j, pl.ds(8 * g, 8), :] = mask[j, pl.ds(8 * g, 8), :].astype(F32)

    by_column = {-1: zl, 0: zp, 1: zr}

    def within(j, share):
        if j == 0:
            share = jnp.where(lane == 0, 0.0, share)
        if j == far:
            share = jnp.where(lane == LANES - 1, 0.0, share)
        return share

    def leaving(g, j):
        here = zp[j, pl.ds(8 * g + 8, 8), :]
        slopes = {}
        for k, (off_row, off_col) in enumerate(OFFSETS):
            beside = by_column[off_col][j, pl.ds(8 * g + 8 + off_row, 8), :]
            slopes[off_row, off_col] = coef[k] * jnp.maximum(here - beside, 0.0)
        share = within(j, 1.0 / (functools.reduce(jnp.add, slopes.values()) + RETENTION))
        recip[j, pl.ds(8 * g + 8, 8), :] = share
        down, up = jnp.where(sub == 7, 0.0, share), jnp.where(sub == 0, 0.0, share)
        out = []
        for c in (-1, 0, 1):
            moved = pltpu.roll(slopes[1, c] * down, 1, 0) + pltpu.roll(slopes[-1, c] * up, 7, 0)
            out.append(moved if c == 0 else moved + slopes[0, c] * share)
        return out

    def across(fields, j):
        west = fields[j - 1][2] if j > 0 else nothing
        east = fields[j + 1][0] if j < far else nothing
        from_west = pltpu.roll(jnp.where(lane == LANES - 1, west, fields[j][2]), 1, 1)
        from_east = pltpu.roll(jnp.where(lane == 0, east, fields[j][0]), LANES - 1, 1)
        kept = fields[j][1] + jnp.where(first, 0.0, from_west) + jnp.where(last, 0.0, from_east)
        return kept, jnp.where(first, from_west, jnp.where(last, from_east, 0.0))

    def settle(g, fields):
        for j in range(blocks):
            inner[j, pl.ds(8 * g, 8), :], outer[j, pl.ds(8 * g, 8), :] = across(fields, j)

    pending[...] = jnp.zeros(pending.shape, F32)

    def step(g, carry):
        fields = [[pending[j, c] for c in range(3)] for j in range(blocks)]
        settle(g - 1, fields)
        for j in range(blocks):
            for c, value in enumerate(leaving(g, j)):
                pending[j, c] = value
        return carry

    lax.fori_loop(1, groups - 1, step, 0)
    settle(groups - 2, [[pending[j, c] for c in range(3)] for j in range(blocks)])

    for k in range(8):
        @pl.when(exists[k])
        def _():
            copies(k, arriving=True).wait_recv()

    def turn(x, step, axis):
        return x if step == 0 else pltpu.roll(x, (-step) % x.shape[axis], axis)

    coarse_at = (16, 0)
    tile_at = (16 + 2 * crows, 2 * crows)
    line_at = (0, 24 + 2 * crows - 16)

    def window(field):
        def beside(right, left):
            a, b = srecv[right, 0:crows, :], srecv[left, 0:crows, :]
            return jnp.where(lane_c < half, a, b) if field == 0 else pltpu.roll(jnp.where(lane_c < half, b, a), half, 1)

        def level(slot):
            return vrecv[slot, coarse_at[slot] + field * crows:coarse_at[slot] + (field + 1) * crows, :]

        here = jnp.concatenate([tall[16 + field * crows:16 + (field + 1) * crows, :], beside(0, 4)], axis=1)
        below = jnp.concatenate([level(0), beside(1, 3)], axis=1)
        above = jnp.concatenate([level(1), beside(7, 5)], axis=1)
        sub_w = lax.broadcasted_iota(jnp.int32, (8, 2 * LANES), 0)
        mixed = jnp.where(sub_w < 4, below[8:16], above[crows - 16:crows - 8])
        return jnp.concatenate([here, below[0:8], mixed, above[crows - 8:crows]], axis=0)

    def shares(z):
        beside_rows = {step: turn(z, step, 1) for step in (-1, 0, 1)}
        return beside_rows

    z = window(0)
    supply = window(1)
    high = z.shape[0]
    beside_z = {step: turn(z, step, 1) for step in (-1, 0, 1)}
    slopes = []
    for k, (step_row, step_col) in enumerate(OFFSETS):
        slopes.append(coef[k] * jnp.maximum(z - turn(beside_z[step_col], step_row, 0), 0.0))
    share = 1.0 / (functools.reduce(jnp.add, slopes) + RETENTION)
    weight = {}
    for k, (step_row, step_col) in enumerate(OFFSETS):
        weight[step_row, step_col] = turn(slopes[k] * share, -step_col, 1)
    flow = supply
    for _ in range(ITERS):
        moved = {step: turn(flow, -step, 1) for step in (-1, 0, 1)}
        sums = {}
        for step_row in (-1, 0, 1):
            sums[step_row] = functools.reduce(
                jnp.add, [weight[step_row, c] * moved[c] for c in (-1, 0, 1) if (step_row, c) in weight])
        flow = supply + sums[0] + turn(sums[1], -1, 0) + turn(sums[-1], 1, 0)

    for slot, sign in ((0, 1), (1, -1)):
        lines = [vrecv[slot, line_at[slot] + 8 * i:line_at[slot] + 8 * i + 8, :] for i in range(2)]
        own_at = 56 + 2 * crows - 24 if slot == 0 else 0
        if slot == 0:
            three = [tall[32 + 2 * crows:40 + 2 * crows, :], lines[0], lines[1]]
            at = rows + 8
        else:
            three = [lines[0], lines[1], tall[0:8, :]]
            at = 7

        def beside_line(x, step):
            moved = pltpu.roll(x, 1 if step < 0 else LANES - 1, 1)
            edge = pltpu.roll(moved, 1 if step < 0 else 7, 0)
            return jnp.where(lane == (0 if step < 0 else LANES - 1), edge, moved)

        near = [{0: x, -1: beside_line(x, -1), 1: beside_line(x, 1)} for x in three]
        total_slope = jnp.full((8, LANES), RETENTION, F32)
        for k, (off_row, off_col) in enumerate(OFFSETS):
            total_slope = total_slope + coef[k] * jnp.maximum(three[1] - near[1 + off_row][off_col], 0.0)
        line_share = 1.0 / total_slope
        line_share = jnp.where(jnp.logical_and(sub == 0, lane == 0), 0.0, line_share)
        line_share = jnp.where(jnp.logical_and(sub == far, lane == LANES - 1), 0.0, line_share)
        for j in range(blocks):
            for step, ref in by_column.items():
                ref[j, at:at + 1, :] = near[1][step][j:j + 1, :]
            recip[j, at:at + 1, :] = line_share[j:j + 1, :]

    for g in (0, groups - 1):
        settle(g, [leaving(g, j) for j in range(blocks)])

    for number, way in enumerate((1, -1)):
        for h in range(halves):
            target = pl.ds(8 + 64 * h + (0 if way == 1 else 7), 8, stride=8)
            source = pl.ds(8 + 64 * h + (-1 if way == 1 else 8), 8, stride=8)
            fields = []
            for j in range(blocks):
                from_z, scale = zp[j, source, :], recip[j, source, :]
                fields.append([
                    coef[OFFSETS.index((way, c))] * jnp.maximum(from_z - by_column[c][j, target, :], 0.0) * scale for c in (-1, 0, 1)])
            for j in range(blocks):
                inner_edge[number, j, 8 * h:8 * h + 8, :], outer_edge[number, j, 8 * h:8 * h + 8, :] = across(fields, j)

    def column(own, left, right):
        beside = jnp.where(sub < 2, pltpu.roll(left, 4, 0), pltpu.roll(right, 4, 0))
        return jnp.where(jnp.logical_and(sub >= 2, sub < 6), own, beside)

    side_tile = [srecv[k, crows:crows + 8, :] for k in range(8)]
    tall_tile = [vrecv[slot, tile_at[slot]:tile_at[slot] + 8, :] for slot in range(2)]
    tile = side[crows:crows + 8, :]
    below = column(tall_tile[0], side_tile[3], side_tile[1])
    above = column(tall_tile[1], side_tile[5], side_tile[7])
    ze = jnp.concatenate([column(tile, side_tile[4], side_tile[0]), jnp.where(lane < half, below, above)], axis=1)
    sub_e = lax.broadcasted_iota(jnp.int32, (8, 2 * LANES), 0)
    beside_e = {step: turn(ze, step, 1) for step in (-1, 0, 1)}
    flux = {}
    for k, (off_row, off_col) in enumerate(OFFSETS):
        flux[off_row, off_col] = coef[k] * jnp.maximum(ze - turn(beside_e[off_row], off_col, 0), 0.0)
    share_e = 1.0 / (functools.reduce(jnp.add, flux.values()) + RETENTION)

    def lines_of(off_row):
        right, left = flux[off_row, 1] * share_e, flux[off_row, -1] * share_e
        picked = jnp.where(sub_e == 1, right, jnp.where(sub_e == 6, left, 0.0))
        picked = jnp.where(sub_e == 3, pltpu.roll(right, 1, 0), jnp.where(sub_e == 4, pltpu.roll(left, 7, 0), picked))
        if off_row == 0:
            return picked
        return jnp.where(jnp.logical_or(sub_e == 2, sub_e == 5), flux[off_row, 0] * share_e, picked)

    from_above = turn(lines_of(1), -1, 1)[:, :LANES]
    from_below = turn(lines_of(-1), 1, 1)[:, :LANES]
    inside = lines_of(0)[:, :LANES] + jnp.where(first, 0.0, from_above) + jnp.where(last, 0.0, from_below)
    outside = jnp.where(first, from_above, jnp.where(last, from_below, 0.0))
    gap = jnp.zeros((LANES - 16, LANES), F32)

    def upright(lines, width):
        if width == 2:
            top = jnp.where(sub < 2, pltpu.roll(lines, 6, 0), 0.0)
            bottom = jnp.where(sub >= 6, pltpu.roll(lines, 2, 0), 0.0)
        else:
            top = jnp.where(sub == 0, pltpu.roll(lines, 7, 0), 0.0)
            bottom = jnp.where(sub == 7, pltpu.roll(lines, 1, 0), 0.0)
        return jnp.transpose(jnp.concatenate([top, gap, bottom], axis=0))

    for field, width in ((inner, 2), (outer, 1)):
        values = upright(inside, width)
        for g in range(groups):
            at = slice(8 * g, 8 * g + 8)
            field[0, at, :] = field[0, at, :] + jnp.where(lane < half, values[at], 0.0)
            field[far, at, :] = field[far, at, :] + jnp.where(lane < half, 0.0, values[at])
    for field, width in ((inner_edge, 2), (outer_edge, 1)):
        turned[width - 1] = upright(outside, width)
        for number in range(2):
            for h in range(halves):
                at = slice(8 * h, 8 * h + 8)
                values = turned[width - 1, pl.ds(64 * h + 7 * number, 8, stride=8), :]
                field[number, 0, at, :] = field[number, 0, at, :] + jnp.where(lane < half, values, 0.0)
                field[number, far, at, :] = field[number, far, at, :] + jnp.where(lane < half, 0.0, values)

    left = turn(flow, -1, 1)[:, :LANES]
    right = turn(flow, 1, 1)[:, :LANES]
    centre = flow[:, :LANES]
    per_block = LANES // 8
    for j in range(blocks):
        index = lane // 8 + j * per_block
        spread = []
        for at in list(range(0, crows, 8)) + [crows, high - 8]:
            mid = take_lanes(centre[at:at + 8], index)
            beside = jnp.where(first, take_lanes(left[at:at + 8], index), take_lanes(right[at:at + 8], index))
            spread.append((mid, beside))
        for h in range(halves):
            for number in range(2):
                terms = []
                for which in range(2):
                    here = spread[h][which]
                    if number == 0:
                        other = spread[h - 1][which] if h > 0 else spread[-1][which]
                        level = jnp.where(sub == 0, pltpu.roll(other, 1, 0), pltpu.roll(here, 1, 0))
                    else:
                        other = spread[h + 1][which] if h < halves - 1 else spread[-2][which]
                        level = jnp.where(sub == 7, pltpu.roll(other, 7, 0), pltpu.roll(here, 7, 0))
                    terms.append((inner_edge, outer_edge)[which][number, j, 8 * h:8 * h + 8, :] * level)
                at = pl.ds(64 * h + 7 * number, 8, stride=8)
                base[j, at, :] = base[j, at, :] + (terms[0] + terms[1])
        for g in range(groups):
            def level(number):
                return jnp.broadcast_to(spread[g // 8][number][g % 8:g % 8 + 1, :], (8, LANES))

            at = slice(8 * g, 8 * g + 8)
            out_ref[at, j * LANES:(j + 1) * LANES] = base[j, at, :] + inner[j, at, :] * level(0) + outer[j, at, :] * level(1)

    for k in range(8):
        @pl.when(exists[k])
        def _():
            copies(k).wait_send()


def solution(mesh):
    row_devices, col_devices = mesh.shape["rows"], mesh.shape["cols"]

    def on_device(elevation, data_mask, tie_order):
        rows, cols = elevation.shape
        groups, blocks = rows // 8, cols // LANES
        tall = 24 + 2 * groups
        return pl.pallas_call(
            functools.partial(kernel, row_devices, col_devices),
            out_shape=pltpu.VMEM((rows, cols), F32),
            in_specs=[pl.BlockSpec(memory_space=pl.ANY)] * 3,
            out_specs=pl.BlockSpec(memory_space=pltpu.VMEM),
            scratch_shapes=[
                pltpu.SMEM((8,), jnp.int32),
                pltpu.VMEM((blocks, rows + 16, LANES), F32),
                pltpu.VMEM((blocks, rows + 16, LANES), F32),
                pltpu.VMEM((blocks, rows + 16, LANES), F32),
                pltpu.VMEM((blocks, rows, LANES), jnp.int32),
                pltpu.VMEM((blocks, rows + 16, LANES), F32),
                pltpu.VMEM((blocks, 3, 8, LANES), F32),
                pltpu.VMEM((blocks, rows, LANES), F32),
                pltpu.VMEM((blocks, rows, LANES), F32),
                pltpu.VMEM((blocks, rows, LANES), F32),
                pltpu.VMEM((2, blocks, groups, LANES), F32),
                pltpu.VMEM((2, blocks, groups, LANES), F32),
                pltpu.VMEM((2, rows, LANES), F32),
                pltpu.VMEM((cols, LANES), jnp.bfloat16),
                pltpu.VMEM((groups + 8, LANES), F32),
                pltpu.VMEM((tall + 16, LANES), F32),
                pltpu.VMEM((8, groups + 8, LANES), F32),
                pltpu.VMEM((2, tall, LANES), F32),
                pltpu.SemaphoreType.DMA((2 * blocks,)),
                pltpu.SemaphoreType.DMA,
                pltpu.SemaphoreType.DMA((8,)),
                pltpu.SemaphoreType.DMA((8,)),
            ],
            compiler_params=pltpu.CompilerParams(collective_id=0, has_side_effects=True, vmem_limit_bytes=61000000),
        )(tie_order, elevation, data_mask)

    return jax.shard_map(
        on_device, mesh=mesh, in_specs=(P("rows", "cols"), P("rows", "cols"), P()),
        out_specs=P("rows", "cols"), check_vma=False)
```

```python
import functools

import jax
import jax.numpy as jnp
from jax import lax
from jax.experimental import pallas as pl
from jax.experimental.pallas import tpu as pltpu
from jax.sharding import PartitionSpec as P

ITERS = 8
OFFSETS = ((0, 1), (1, 1), (1, 0), (1, -1), (0, -1), (-1, -1), (-1, 0), (-1, 1))
RECIPROCAL = (1.0, 0.7071067811865476) * 4
RETENTION = 0.1
OUTSIDE = 1000.0
LANES = 128
F32 = jnp.float32


def coefficients(tie_ref):
    out = []
    for k in range(8):
        value = jnp.float32(0.0)
        for i in range(8):
            place = jnp.float32((1.0 + 0.5 * (7.0 - i) / 7.0) * RECIPROCAL[k])
            value = jnp.where(tie_ref[i] == k, place, value)
        out.append(value)
    return out


def shift_lanes(before, here, after, step, lane):
    if step == 0:
        return here
    if step < 0:
        return pltpu.roll(jnp.where(lane == LANES - 1, before, here), 1, 1)
    return pltpu.roll(jnp.where(lane == 0, after, here), LANES - 1, 1)


def take_lanes(values, index):
    return jnp.take_along_axis(values, index, axis=1, mode="promise_in_bounds")


def kernel(row_devices, col_devices, tie_hbm, elev_ref, mask_ref, out_ref, tie_ref, zp, zl, zr, mask, recip, base, inner, outer,
           inner_edge, outer_edge, turned, ones, sums, side, tall, srecv, vrecv, load_sem, tie_sem, send_sem, recv_sem):
    rows, cols = elev_ref.shape
    groups, blocks = rows // 8, cols // LANES
    crows, halves = groups, groups // 8
    row, col = lax.axis_index("rows"), lax.axis_index("cols")
    far = blocks - 1

    loads = {}
    for j in [0, far] + list(range(1, far)):
        part = pl.ds(j * LANES, LANES)
        loads[j] = (
            pltpu.make_async_copy(elev_ref.at[:, part], zp.at[j, pl.ds(8, rows), :], load_sem.at[j]),
            pltpu.make_async_copy(mask_ref.at[:, part], mask.at[j], load_sem.at[blocks + j]))
        loads[j][0].start()
        loads[j][1].start()
    tie_load = pltpu.make_async_copy(tie_hbm, tie_ref, tie_sem)
    tie_load.start()

    barrier = pltpu.get_barrier_semaphore()
    exists = []
    for step_row, step_col in OFFSETS:
        there = jnp.bool_(True)
        if step_row > 0:
            there = row < row_devices - 1
        if step_row < 0:
            there = row > 0
        if step_col > 0:
            there = jnp.logical_and(there, col < col_devices - 1)
        if step_col < 0:
            there = jnp.logical_and(there, col > 0)
        exists.append(there)

    def peer(k):
        return {"rows": row + OFFSETS[k][0], "cols": col + OFFSETS[k][1]}

    for k in range(8):
        @pl.when(exists[k])
        def _():
            pl.semaphore_signal(barrier, inc=1, device_id=peer(k), device_id_type=pl.DeviceIdType.MESH)

    lane = lax.broadcasted_iota(jnp.int32, (8, LANES), 1)
    sub = lax.broadcasted_iota(jnp.int32, (8, LANES), 0)
    first, last = (lane & 7) == 0, (lane & 7) == 7
    half = LANES // 2
    nothing = jnp.zeros((8, LANES), F32)

    SIDES, UPDOWN = (0, 1, 3, 4, 5, 7), (2, 6)

    ones[...] = (
        lax.broadcasted_iota(jnp.int32, (cols, LANES), 0) // 8 == lax.broadcasted_iota(jnp.int32, (cols, LANES), 1)
    ).astype(F32).astype(jnp.bfloat16)

    order = list(loads)

    def row_sums(some):
        for j in some:
            height_sum = jnp.zeros((crows, LANES), F32)
            count_sum = jnp.zeros((crows, LANES), F32)
            for s in range(8):
                valid = mask[j, pl.ds(s, crows, stride=8), :].astype(F32)
                height_sum = height_sum + valid * zp[j, pl.ds(8 + s, crows, stride=8), :]
                count_sum = count_sum + valid
            high = height_sum.astype(jnp.bfloat16)
            rest = height_sum - high.astype(F32)
            middle = rest.astype(jnp.bfloat16)
            low = (rest - middle.astype(F32)).astype(jnp.bfloat16)
            sums[:, j * LANES:(j + 1) * LANES] = jnp.concatenate([count_sum.astype(jnp.bfloat16), high, middle, low], axis=0)
            for number, at in enumerate((8, 9, rows + 6, rows + 7)):
                line = (0, 8, 24 + 2 * crows, 32 + 2 * crows)[number]
                tall[line + j:line + j + 1, :] = zp[j, at:at + 1, :]

    for part in (order[:blocks // 2], order[blocks // 2:]):
        for j in part:
            loads[j][0].wait()
            loads[j][1].wait()
        if 0 in part:
            ends = jnp.where(lax.broadcasted_iota(jnp.int32, (rows, LANES), 1) < half, zp[0, 8:8 + rows, :], zp[far, 8:8 + rows, :])
            ends = jnp.transpose(ends)
            tile = jnp.where(sub < 4, pltpu.roll(ends[0:8], 2, 0), pltpu.roll(ends[LANES - 8:LANES], 6, 0))
            tall[16 + 2 * crows:24 + 2 * crows, :] = tile
        row_sums(part)
    total = jnp.dot(sums[...], ones[...], preferred_element_type=F32)
    counts = total[0:crows]
    heights = total[crows:2 * crows] + (total[2 * crows:3 * crows] + total[3 * crows:])
    overview = heights / (counts + 1.0)
    runoff = counts * (1.0 / 64.0)
    tall[16:16 + crows, :] = overview
    tall[16 + crows:16 + 2 * crows, :] = runoff

    quarter, place = lane // 32, lane & 15
    early = (lane & 31) < 16
    eastward, westward = [], []
    for h in range(halves):
        at = slice(8 * h, 8 * h + 8)
        height = take_lanes(overview[at], jnp.where(early, LANES - 16, 0) + place)
        count = take_lanes(runoff[at], jnp.where(early, 0, LANES - 16) + place)
        for whole, value in ((eastward, jnp.where(early, height, count)), (westward, jnp.where(early, count, height))):
            whole += [value, pltpu.roll(value, 4, 0)]

    def quarters(whole):
        return jnp.where(quarter < 2, jnp.where(quarter == 0, whole[0], whole[1]), jnp.where(quarter == 2, whole[2], whole[3]))

    tile = tall[16 + 2 * crows:24 + 2 * crows, :]
    side[0] = jnp.where(sub < 4, quarters(eastward), tile)
    side[1] = jnp.where(sub < 4, tile, quarters(westward))

    pl.semaphore_wait(barrier, functools.reduce(jnp.add, [there.astype(jnp.int32) for there in exists]))

    def copies(k, arriving=False):
        slot = k if arriving else (k + 4) % 8
        if k in UPDOWN:
            src, dst = tall.at[pl.ds(16 if k == 2 else 0, 24 + 2 * crows), :], vrecv.at[slot // 4]
        else:
            src, dst = side.at[0 if OFFSETS[k][1] > 0 else 1], srecv.at[slot]
        return pltpu.make_async_remote_copy(
            src_ref=src, dst_ref=dst, send_sem=send_sem.at[k], recv_sem=recv_sem.at[slot],
            device_id=peer(k), device_id_type=pl.DeviceIdType.MESH)

    for k in (1, 3, 5, 7, 0, 4, 2, 6):
        @pl.when(exists[k])
        def _():
            copies(k).start()

    for k in range(8):
        @pl.when(jnp.logical_not(exists[k]))
        def _():
            if k in UPDOWN:
                for at in range(0, 24 + 2 * crows, 8):
                    start = 16 + crows if k == 2 else crows
                    vrecv[k // 4, at:at + 8, :] = jnp.full((8, LANES), 0.0 if start <= at < start + crows else OUTSIDE, F32)
            else:
                empty = jnp.logical_and(early, sub >= 4) if OFFSETS[k][1] > 0 else jnp.logical_and(jnp.logical_not(early), sub < 4)
                srecv[k] = jnp.where(empty, 0.0, OUTSIDE)

    tie_load.wait()
    coef = coefficients(tie_ref)

    for g in range(groups):
        at = pl.ds(8 * g + 8, 8)
        for j in range(blocks):
            here = zp[j, at, :]
            before, after = zp[(j - 1) % blocks, at, :], zp[(j + 1) % blocks, at, :]
            zl[j, at, :] = shift_lanes(before, here, after, -1, lane)
            zr[j, at, :] = shift_lanes(before, here, after, 1, lane)
            base[j, pl.ds(8 * g, 8), :] = mask[j, pl.ds(8 * g, 8), :].astype(F32)

    by_column = {-1: zl, 0: zp, 1: zr}

    def within(j, share):
        if j == 0:
            share = jnp.where(lane == 0, 0.0, share)
        if j == far:
            share = jnp.where(lane == LANES - 1, 0.0, share)
        return share

    def leaving(g, j):
        here = zp[j, pl.ds(8 * g + 8, 8), :]
        slopes = {}
        for k, (off_row, off_col) in enumerate(OFFSETS):
            beside = by_column[off_col][j, pl.ds(8 * g + 8 + off_row, 8), :]
            slopes[off_row, off_col] = coef[k] * jnp.maximum(here - beside, 0.0)
        share = within(j, 1.0 / (functools.reduce(jnp.add, slopes.values()) + RETENTION))
        recip[j, pl.ds(8 * g + 8, 8), :] = share
        down, up = jnp.where(sub == 7, 0.0, share), jnp.where(sub == 0, 0.0, share)
        out = []
        for c in (-1, 0, 1):
            moved = pltpu.roll(slopes[1, c] * down, 1, 0) + pltpu.roll(slopes[-1, c] * up, 7, 0)
            out.append(moved if c == 0 else moved + slopes[0, c] * share)
        return out

    def across(fields, j):
        west = fields[j - 1][2] if j > 0 else nothing
        east = fields[j + 1][0] if j < far else nothing
        from_west = pltpu.roll(jnp.where(lane == LANES - 1, west, fields[j][2]), 1, 1)
        from_east = pltpu.roll(jnp.where(lane == 0, east, fields[j][0]), LANES - 1, 1)
        kept = fields[j][1] + jnp.where(first, 0.0, from_west) + jnp.where(last, 0.0, from_east)
        return kept, jnp.where(first, from_west, jnp.where(last, from_east, 0.0))

    def settle(g, fields):
        for j in range(blocks):
            inner[j, pl.ds(8 * g, 8), :], outer[j, pl.ds(8 * g, 8), :] = across(fields, j)

    for g in range(1, groups - 1):
        settle(g, [leaving(g, j) for j in range(blocks)])

    for k in range(8):
        @pl.when(exists[k])
        def _():
            copies(k, arriving=True).wait_recv()

    def turn(x, step, axis):
        return x if step == 0 else pltpu.roll(x, (-step) % x.shape[axis], axis)

    coarse_at = (16, 0)
    tile_at = (16 + 2 * crows, 2 * crows)
    line_at = (0, 24 + 2 * crows - 16)

    def window(field):
        def unpacked(k, h):
            given = srecv[k]
            swapped = pltpu.roll(given, 4, 0)
            if OFFSETS[k][1] > 0:
                start, first_rows, last_rows = 16 * (1 - field), swapped, given
            else:
                start, first_rows, last_rows = 16 * field + 16, given, swapped
            return jnp.where(
                sub < 4, turn(first_rows, start + 64 * h + (32 if OFFSETS[k][1] > 0 else 0), 1),
                turn(last_rows, start + 64 * h + (0 if OFFSETS[k][1] > 0 else 32), 1))

        def beside(right, left):
            return jnp.concatenate([jnp.where(lane < half, unpacked(right, h), unpacked(left, h)) for h in range(halves)], axis=0)

        def level(slot):
            return vrecv[slot, coarse_at[slot] + field * crows:coarse_at[slot] + (field + 1) * crows, :]

        here = jnp.concatenate([tall[16 + field * crows:16 + (field + 1) * crows, :], beside(0, 4)], axis=1)
        below = jnp.concatenate([level(0), beside(1, 3)], axis=1)
        above = jnp.concatenate([level(1), beside(7, 5)], axis=1)
        sub_w = lax.broadcasted_iota(jnp.int32, (8, 2 * LANES), 0)
        mixed = jnp.where(sub_w < 4, below[8:16], above[crows - 16:crows - 8])
        return jnp.concatenate([here, below[0:8], mixed, above[crows - 8:crows]], axis=0)

    z = window(0)
    supply = window(1)
    high = z.shape[0]
    beside_z = {step: turn(z, step, 1) for step in (-1, 0, 1)}
    slopes = []
    for k, (step_row, step_col) in enumerate(OFFSETS):
        slopes.append(coef[k] * jnp.maximum(z - turn(beside_z[step_col], step_row, 0), 0.0))
    share = 1.0 / (functools.reduce(jnp.add, slopes) + RETENTION)
    weight = {}
    for k, (step_row, step_col) in enumerate(OFFSETS):
        weight[step_row, step_col] = turn(slopes[k] * share, -step_col, 1)
    flow = supply
    for _ in range(ITERS):
        moved = {step: turn(flow, -step, 1) for step in (-1, 0, 1)}
        sums = {}
        for step_row in (-1, 0, 1):
            sums[step_row] = functools.reduce(
                jnp.add, [weight[step_row, c] * moved[c] for c in (-1, 0, 1) if (step_row, c) in weight])
        flow = supply + sums[0] + turn(sums[1], -1, 0) + turn(sums[-1], 1, 0)

    for slot, sign in ((0, 1), (1, -1)):
        lines = [vrecv[slot, line_at[slot] + 8 * i:line_at[slot] + 8 * i + 8, :] for i in range(2)]
        if slot == 0:
            three = [tall[32 + 2 * crows:40 + 2 * crows, :], lines[0], lines[1]]
            at = rows + 8
        else:
            three = [lines[0], lines[1], tall[0:8, :]]
            at = 7

        def beside_line(x, step):
            moved = pltpu.roll(x, 1 if step < 0 else LANES - 1, 1)
            edge = pltpu.roll(moved, 1 if step < 0 else 7, 0)
            return jnp.where(lane == (0 if step < 0 else LANES - 1), edge, moved)

        near = [{0: x, -1: beside_line(x, -1), 1: beside_line(x, 1)} for x in three]
        total_slope = jnp.full((8, LANES), RETENTION, F32)
        for k, (off_row, off_col) in enumerate(OFFSETS):
            total_slope = total_slope + coef[k] * jnp.maximum(three[1] - near[1 + off_row][off_col], 0.0)
        line_share = 1.0 / total_slope
        line_share = jnp.where(jnp.logical_and(sub == 0, lane == 0), 0.0, line_share)
        line_share = jnp.where(jnp.logical_and(sub == far, lane == LANES - 1), 0.0, line_share)
        for j in range(blocks):
            for step, ref in by_column.items():
                ref[j, at:at + 1, :] = near[1][step][j:j + 1, :]
            recip[j, at:at + 1, :] = line_share[j:j + 1, :]

    for g in (0, groups - 1):
        settle(g, [leaving(g, j) for j in range(blocks)])

    for number, way in enumerate((1, -1)):
        for h in range(halves):
            target = pl.ds(8 + 64 * h + (0 if way == 1 else 7), 8, stride=8)
            source = pl.ds(8 + 64 * h + (-1 if way == 1 else 8), 8, stride=8)
            fields = []
            for j in range(blocks):
                from_z, scale = zp[j, source, :], recip[j, source, :]
                fields.append([
                    coef[OFFSETS.index((way, c))] * jnp.maximum(from_z - by_column[c][j, target, :], 0.0) * scale for c in (-1, 0, 1)])
            for j in range(blocks):
                inner_edge[number, j, 8 * h:8 * h + 8, :], outer_edge[number, j, 8 * h:8 * h + 8, :] = across(fields, j)

    def column(own, left, right):
        beside = jnp.where(sub < 2, pltpu.roll(left, 4, 0), pltpu.roll(right, 4, 0))
        return jnp.where(jnp.logical_and(sub >= 2, sub < 6), own, beside)

    side_tile = [srecv[k] for k in range(8)]
    tall_tile = [vrecv[slot, tile_at[slot]:tile_at[slot] + 8, :] for slot in range(2)]
    tile = tall[16 + 2 * crows:24 + 2 * crows, :]
    below = column(tall_tile[0], side_tile[3], side_tile[1])
    above = column(tall_tile[1], side_tile[5], side_tile[7])
    ze = jnp.concatenate([column(tile, side_tile[4], side_tile[0]), jnp.where(lane < half, below, above)], axis=1)
    sub_e = lax.broadcasted_iota(jnp.int32, (8, 2 * LANES), 0)
    beside_e = {step: turn(ze, step, 1) for step in (-1, 0, 1)}
    flux = {}
    for k, (off_row, off_col) in enumerate(OFFSETS):
        flux[off_row, off_col] = coef[k] * jnp.maximum(ze - turn(beside_e[off_row], off_col, 0), 0.0)
    share_e = 1.0 / (functools.reduce(jnp.add, flux.values()) + RETENTION)

    def lines_of(off_row):
        right, left = flux[off_row, 1] * share_e, flux[off_row, -1] * share_e
        picked = jnp.where(sub_e == 1, right, jnp.where(sub_e == 6, left, 0.0))
        picked = jnp.where(sub_e == 3, pltpu.roll(right, 1, 0), jnp.where(sub_e == 4, pltpu.roll(left, 7, 0), picked))
        if off_row == 0:
            return picked
        return jnp.where(jnp.logical_or(sub_e == 2, sub_e == 5), flux[off_row, 0] * share_e, picked)

    from_above = turn(lines_of(1), -1, 1)[:, :LANES]
    from_below = turn(lines_of(-1), 1, 1)[:, :LANES]
    inside = lines_of(0)[:, :LANES] + jnp.where(first, 0.0, from_above) + jnp.where(last, 0.0, from_below)
    outside = jnp.where(first, from_above, jnp.where(last, from_below, 0.0))
    gap = jnp.zeros((LANES - 16, LANES), F32)

    def upright(lines, width):
        if width == 2:
            top = jnp.where(sub < 2, pltpu.roll(lines, 6, 0), 0.0)
            bottom = jnp.where(sub >= 6, pltpu.roll(lines, 2, 0), 0.0)
        else:
            top = jnp.where(sub == 0, pltpu.roll(lines, 7, 0), 0.0)
            bottom = jnp.where(sub == 7, pltpu.roll(lines, 1, 0), 0.0)
        return jnp.transpose(jnp.concatenate([top, gap, bottom], axis=0))

    for field, width in ((inner, 2), (outer, 1)):
        values = upright(inside, width)
        for g in range(groups):
            at = slice(8 * g, 8 * g + 8)
            field[0, at, :] = field[0, at, :] + jnp.where(lane < half, values[at], 0.0)
            field[far, at, :] = field[far, at, :] + jnp.where(lane < half, 0.0, values[at])
    for field, width in ((inner_edge, 2), (outer_edge, 1)):
        turned[width - 1] = upright(outside, width)
        for number in range(2):
            for h in range(halves):
                at = slice(8 * h, 8 * h + 8)
                values = turned[width - 1, pl.ds(64 * h + 7 * number, 8, stride=8), :]
                field[number, 0, at, :] = field[number, 0, at, :] + jnp.where(lane < half, values, 0.0)
                field[number, far, at, :] = field[number, far, at, :] + jnp.where(lane < half, 0.0, values)

    left = turn(flow, -1, 1)[:, :LANES]
    right = turn(flow, 1, 1)[:, :LANES]
    centre = flow[:, :LANES]
    per_block = LANES // 8
    for j in range(blocks):
        index = lane // 8 + j * per_block
        spread = []
        for at in list(range(0, crows, 8)) + [crows, high - 8]:
            mid = take_lanes(centre[at:at + 8], index)
            beside = jnp.where(first, take_lanes(left[at:at + 8], index), take_lanes(right[at:at + 8], index))
            spread.append((mid, beside))
        for h in range(halves):
            for number in range(2):
                terms = []
                for which in range(2):
                    here = spread[h][which]
                    if number == 0:
                        other = spread[h - 1][which] if h > 0 else spread[-1][which]
                        level = jnp.where(sub == 0, pltpu.roll(other, 1, 0), pltpu.roll(here, 1, 0))
                    else:
                        other = spread[h + 1][which] if h < halves - 1 else spread[-2][which]
                        level = jnp.where(sub == 7, pltpu.roll(other, 7, 0), pltpu.roll(here, 7, 0))
                    terms.append((inner_edge, outer_edge)[which][number, j, 8 * h:8 * h + 8, :] * level)
                at = pl.ds(64 * h + 7 * number, 8, stride=8)
                base[j, at, :] = base[j, at, :] + (terms[0] + terms[1])
        for g in range(groups):
            def level(number):
                return jnp.broadcast_to(spread[g // 8][number][g % 8:g % 8 + 1, :], (8, LANES))

            at = slice(8 * g, 8 * g + 8)
            out_ref[at, j * LANES:(j + 1) * LANES] = base[j, at, :] + inner[j, at, :] * level(0) + outer[j, at, :] * level(1)

    for k in range(8):
        @pl.when(exists[k])
        def _():
            copies(k).wait_send()


def solution(mesh):
    row_devices, col_devices = mesh.shape["rows"], mesh.shape["cols"]

    def on_device(elevation, data_mask, tie_order):
        rows, cols = elevation.shape
        groups, blocks = rows // 8, cols // LANES
        tall = 24 + 2 * groups
        return pl.pallas_call(
            functools.partial(kernel, row_devices, col_devices),
            out_shape=pltpu.VMEM((rows, cols), F32),
            in_specs=[pl.BlockSpec(memory_space=pl.ANY)] * 3,
            out_specs=pl.BlockSpec(memory_space=pltpu.VMEM),
            scratch_shapes=[
                pltpu.SMEM((8,), jnp.int32),
                pltpu.VMEM((blocks, rows + 16, LANES), F32),
                pltpu.VMEM((blocks, rows + 16, LANES), F32),
                pltpu.VMEM((blocks, rows + 16, LANES), F32),
                pltpu.VMEM((blocks, rows, LANES), jnp.int32),
                pltpu.VMEM((blocks, rows + 16, LANES), F32),
                pltpu.VMEM((blocks, rows, LANES), F32),
                pltpu.VMEM((blocks, rows, LANES), F32),
                pltpu.VMEM((blocks, rows, LANES), F32),
                pltpu.VMEM((2, blocks, groups, LANES), F32),
                pltpu.VMEM((2, blocks, groups, LANES), F32),
                pltpu.VMEM((2, rows, LANES), F32),
                pltpu.VMEM((cols, LANES), jnp.bfloat16),
                pltpu.VMEM((4 * groups, cols), jnp.bfloat16),
                pltpu.VMEM((2, 8, LANES), F32),
                pltpu.VMEM((tall + 16, LANES), F32),
                pltpu.VMEM((8, 8, LANES), F32),
                pltpu.VMEM((2, tall, LANES), F32),
                pltpu.SemaphoreType.DMA((2 * blocks,)),
                pltpu.SemaphoreType.DMA,
                pltpu.SemaphoreType.DMA((8,)),
                pltpu.SemaphoreType.DMA((8,)),
            ],
            compiler_params=pltpu.CompilerParams(collective_id=0, has_side_effects=True, vmem_limit_bytes=61000000),
        )(tie_order, elevation, data_mask)

    return jax.shard_map(
        on_device, mesh=mesh, in_specs=(P("rows", "cols"), P("rows", "cols"), P()),
        out_specs=P("rows", "cols"), check_vma=False)
```

```python
import functools

import jax
import jax.numpy as jnp
from jax import lax
from jax.experimental import pallas as pl
from jax.experimental.pallas import tpu as pltpu
from jax.sharding import PartitionSpec as P

ITERS = 8
OFFSETS = ((0, 1), (1, 1), (1, 0), (1, -1), (0, -1), (-1, -1), (-1, 0), (-1, 1))
RECIPROCAL = (1.0, 0.7071067811865476) * 4
RETENTION = 0.1
OUTSIDE = 1000.0
LANES = 128
F32 = jnp.float32


def coefficients(tie_ref):
    out = []
    for k in range(8):
        value = jnp.float32(0.0)
        for i in range(8):
            place = jnp.float32((1.0 + 0.5 * (7.0 - i) / 7.0) * RECIPROCAL[k])
            value = jnp.where(tie_ref[i] == k, place, value)
        out.append(value)
    return out


def shift_lanes(before, here, after, step, lane):
    if step == 0:
        return here
    if step < 0:
        return pltpu.roll(jnp.where(lane == LANES - 1, before, here), 1, 1)
    return pltpu.roll(jnp.where(lane == 0, after, here), LANES - 1, 1)


def take_lanes(values, index):
    return jnp.take_along_axis(values, index, axis=1, mode="promise_in_bounds")


def exchange(row_devices, col_devices, tie_hbm, elev_ref, mask_ref, flow_ref, base, inner, outer, inner_edge, outer_edge,
             tie_ref, zp, zl, zr, mask, recip, turned, ones, sums, side, tall, srecv, vrecv, load_sem, tie_sem, send_sem, recv_sem):
    rows, cols = elev_ref.shape
    groups, blocks = rows // 8, cols // LANES
    crows, halves = groups, groups // 8
    row, col = lax.axis_index("rows"), lax.axis_index("cols")
    far = blocks - 1

    loads = {}
    for j in [0, far] + list(range(1, far)):
        part = pl.ds(j * LANES, LANES)
        loads[j] = (
            pltpu.make_async_copy(elev_ref.at[:, part], zp.at[j, pl.ds(8, rows), :], load_sem.at[j]),
            pltpu.make_async_copy(mask_ref.at[:, part], mask.at[j], load_sem.at[blocks + j]))
        loads[j][0].start()
        loads[j][1].start()
    tie_load = pltpu.make_async_copy(tie_hbm, tie_ref, tie_sem)
    tie_load.start()

    barrier = pltpu.get_barrier_semaphore()
    exists = []
    for step_row, step_col in OFFSETS:
        there = jnp.bool_(True)
        if step_row > 0:
            there = row < row_devices - 1
        if step_row < 0:
            there = row > 0
        if step_col > 0:
            there = jnp.logical_and(there, col < col_devices - 1)
        if step_col < 0:
            there = jnp.logical_and(there, col > 0)
        exists.append(there)

    def peer(k):
        return {"rows": row + OFFSETS[k][0], "cols": col + OFFSETS[k][1]}

    for k in range(8):
        @pl.when(exists[k])
        def _():
            pl.semaphore_signal(barrier, inc=1, device_id=peer(k), device_id_type=pl.DeviceIdType.MESH)

    lane = lax.broadcasted_iota(jnp.int32, (8, LANES), 1)
    sub = lax.broadcasted_iota(jnp.int32, (8, LANES), 0)
    first, last = (lane & 7) == 0, (lane & 7) == 7
    lane_c = lax.broadcasted_iota(jnp.int32, (crows, LANES), 1)
    middle_lanes = jnp.logical_and(lane_c >= LANES // 4, lane_c < 3 * LANES // 4)
    half = LANES // 2
    nothing = jnp.zeros((8, LANES), F32)

    SIDES, UPDOWN = (0, 1, 3, 4, 5, 7), (2, 6)

    taker = lax.broadcasted_iota(jnp.int32, (cols, LANES), 1)
    giver = lax.broadcasted_iota(jnp.int32, (cols, LANES), 0) // 8
    ones[:, :LANES] = (giver == taker).astype(F32).astype(jnp.bfloat16)
    ones[:, LANES:] = (giver == (taker ^ half)).astype(F32).astype(jnp.bfloat16)

    order = list(loads)

    def row_sums(some):
        for j in some:
            height_sum = jnp.zeros((crows, LANES), F32)
            count_sum = jnp.zeros((crows, LANES), F32)
            for s in range(8):
                valid = mask[j, pl.ds(s, crows, stride=8), :].astype(F32)
                height_sum = height_sum + valid * zp[j, pl.ds(8 + s, crows, stride=8), :]
                count_sum = count_sum + valid
            high = height_sum.astype(jnp.bfloat16)
            rest = height_sum - high.astype(F32)
            middle = rest.astype(jnp.bfloat16)
            low = (rest - middle.astype(F32)).astype(jnp.bfloat16)
            sums[:, j * LANES:(j + 1) * LANES] = jnp.concatenate([count_sum.astype(jnp.bfloat16), high, middle, low], axis=0)
            for number, at in enumerate((8, 9, rows + 6, rows + 7)):
                line = (0, 8, 24 + 2 * crows, 32 + 2 * crows)[number]
                tall[line + j:line + j + 1, :] = zp[j, at:at + 1, :]

    for part in [order[at:at + 2] for at in range(0, blocks, 2)]:
        for j in part:
            loads[j][0].wait()
            loads[j][1].wait()
        if 0 in part:
            ends = jnp.where(lax.broadcasted_iota(jnp.int32, (rows, LANES), 1) < half, zp[0, 8:8 + rows, :], zp[far, 8:8 + rows, :])
            ends = jnp.transpose(ends)
            tile = jnp.where(sub < 4, pltpu.roll(ends[0:8], 2, 0), pltpu.roll(ends[LANES - 8:LANES], 6, 0))
            tall[16 + 2 * crows:24 + 2 * crows, :] = tile
            side[crows:crows + 8, :] = tile
        row_sums(part)
    both = jnp.dot(sums[...], ones[...], preferred_element_type=F32)
    total = both[:, :LANES]
    counts = total[0:crows]
    heights = total[crows:2 * crows] + (total[2 * crows:3 * crows] + total[3 * crows:])
    overview = heights / (counts + 1.0)
    runoff = counts * (1.0 / 64.0)
    tall[16:16 + crows, :] = overview
    tall[16 + crows:16 + 2 * crows, :] = runoff

    side[0:crows, :] = jnp.where(middle_lanes, both[0:crows, LANES:] * (1.0 / 64.0), overview)

    pl.semaphore_wait(barrier, functools.reduce(jnp.add, [there.astype(jnp.int32) for there in exists]))

    def copies(k, arriving=False):
        slot = k if arriving else (k + 4) % 8
        if k in UPDOWN:
            src, dst = tall.at[pl.ds(16 if k == 2 else 0, 24 + 2 * crows), :], vrecv.at[slot // 4]
        else:
            src, dst = side, srecv.at[slot]
        return pltpu.make_async_remote_copy(
            src_ref=src, dst_ref=dst, send_sem=send_sem.at[k], recv_sem=recv_sem.at[slot],
            device_id=peer(k), device_id_type=pl.DeviceIdType.MESH)

    for k in (5, 4, 6, 7, 3, 1, 0, 2):
        @pl.when(exists[k])
        def _():
            copies(k).start()

    for k in range(8):
        @pl.when(jnp.logical_not(exists[k]))
        def _():
            if k in UPDOWN:
                for at in range(0, 24 + 2 * crows, 8):
                    start = 16 + crows if k == 2 else crows
                    vrecv[k // 4, at:at + 8, :] = jnp.full((8, LANES), 0.0 if start <= at < start + crows else OUTSIDE, F32)
            else:
                srecv[k, 0:crows, :] = jnp.where(middle_lanes, 0.0, OUTSIDE)
                srecv[k, crows:crows + 8, :] = jnp.full((8, LANES), OUTSIDE, F32)

    tie_load.wait()
    coef = coefficients(tie_ref)

    for ref in (zp, zl, zr, recip):
        for j in range(blocks):
            ref[j, 0:8, :], ref[j, 8 + rows:16 + rows, :] = nothing, nothing

    for g in range(groups):
        at = pl.ds(8 * g + 8, 8)
        for j in range(blocks):
            here = zp[j, at, :]
            before, after = zp[(j - 1) % blocks, at, :], zp[(j + 1) % blocks, at, :]
            zl[j, at, :] = shift_lanes(before, here, after, -1, lane)
            zr[j, at, :] = shift_lanes(before, here, after, 1, lane)
            base[j, pl.ds(8 * g, 8), :] = mask[j, pl.ds(8 * g, 8), :].astype(F32)

    by_column = {-1: zl, 0: zp, 1: zr}

    def within(j, share):
        if j == 0:
            share = jnp.where(lane == 0, 0.0, share)
        if j == far:
            share = jnp.where(lane == LANES - 1, 0.0, share)
        return share

    def leaving(g, j):
        here = zp[j, pl.ds(8 * g + 8, 8), :]
        slopes = {}
        for k, (off_row, off_col) in enumerate(OFFSETS):
            beside = by_column[off_col][j, pl.ds(8 * g + 8 + off_row, 8), :]
            slopes[off_row, off_col] = coef[k] * jnp.maximum(here - beside, 0.0)
        share = within(j, 1.0 / (functools.reduce(jnp.add, slopes.values()) + RETENTION))
        if g == 0:
            share = jnp.where(sub == 0, 0.0, share)
        if g == groups - 1:
            share = jnp.where(sub == 7, 0.0, share)
        recip[j, pl.ds(8 * g + 8, 8), :] = share
        down, up = jnp.where(sub == 7, 0.0, share), jnp.where(sub == 0, 0.0, share)
        out = []
        for c in (-1, 0, 1):
            moved = pltpu.roll(slopes[1, c] * down, 1, 0) + pltpu.roll(slopes[-1, c] * up, 7, 0)
            out.append(moved if c == 0 else moved + slopes[0, c] * share)
        return out

    def across(fields, j):
        west = fields[j - 1][2] if j > 0 else nothing
        east = fields[j + 1][0] if j < far else nothing
        from_west = pltpu.roll(jnp.where(lane == LANES - 1, west, fields[j][2]), 1, 1)
        from_east = pltpu.roll(jnp.where(lane == 0, east, fields[j][0]), LANES - 1, 1)
        kept = fields[j][1] + jnp.where(first, 0.0, from_west) + jnp.where(last, 0.0, from_east)
        return kept, jnp.where(first, from_west, jnp.where(last, from_east, 0.0))

    def settle(g, fields):
        for j in range(blocks):
            at = pl.ds(j * rows + 8 * g, 8)
            inner[at, :], outer[at, :] = across(fields, j)

    for g in range(groups):
        settle(g, [leaving(g, j) for j in range(blocks)])

    def edge_at(number, j, h):
        return pl.ds((number * blocks + j) * groups + 8 * h, 8)

    def compact(number, way, h):
        target = pl.ds(8 + 64 * h + (0 if way == 1 else 7), 8, stride=8)
        source = pl.ds(8 + 64 * h + (-1 if way == 1 else 8), 8, stride=8)
        fields = []
        for j in range(blocks):
            from_z, scale = zp[j, source, :], recip[j, source, :]
            fields.append([
                coef[OFFSETS.index((way, c))] * jnp.maximum(from_z - by_column[c][j, target, :], 0.0) * scale for c in (-1, 0, 1)])
        for j in range(blocks):
            at = edge_at(number, j, h)
            inner_edge[at, :], outer_edge[at, :] = across(fields, j)

    for number, way in enumerate((1, -1)):
        for h in range(halves):
            compact(number, way, h)

    for k in range(8):
        @pl.when(exists[k])
        def _():
            copies(k, arriving=True).wait_recv()

    def turn(x, step, axis):
        return x if step == 0 else pltpu.roll(x, (-step) % x.shape[axis], axis)

    coarse_at = (16, 0)
    tile_at = (16 + 2 * crows, 2 * crows)
    line_at = (0, 24 + 2 * crows - 16)

    def stacked(of_place):
        end = halves - 1
        rows_of = [of_place(None, h) for h in range(halves)] + [of_place(0, 0)]
        return jnp.concatenate(rows_of + [jnp.where(sub < 4, of_place(0, 1), of_place(1, end - 1)), of_place(1, end)], axis=0)

    def middle_of(field):
        def of_place(slot, h):
            if slot is None:
                return tall[16 + field * crows + 8 * h:24 + field * crows + 8 * h, :]
            return vrecv[slot, coarse_at[slot] + field * crows + 8 * h:coarse_at[slot] + field * crows + 8 * h + 8, :]

        return stacked(of_place)

    def beside_of(east):
        ks = {None: 0 if east else 4, 0: 1 if east else 3, 1: 7 if east else 5}
        return stacked(lambda slot, h: srecv[ks[slot], 8 * h:8 * h + 8, :])

    east, west = beside_of(True), beside_of(False)
    nearer = lax.broadcasted_iota(jnp.int32, east.shape, 1) < half
    z = jnp.concatenate([middle_of(0), jnp.where(nearer, east, west)], axis=1)
    supply = jnp.concatenate([middle_of(1), pltpu.roll(jnp.where(nearer, west, east), half, 1)], axis=1)
    beside_z = {step: turn(z, step, 1) for step in (-1, 0, 1)}
    slopes = []
    for k, (step_row, step_col) in enumerate(OFFSETS):
        slopes.append(coef[k] * jnp.maximum(beside_z[0] - turn(beside_z[step_col], step_row, 0), 0.0))
    share = 1.0 / (functools.reduce(jnp.add, slopes) + RETENTION)

    def core(x):
        return jnp.concatenate([x[0:crows + 8], x[crows + 16:]], axis=0)

    weight = {}
    given = {-1: 0.0, 0: 0.0, 1: 0.0}
    for k, (step_row, step_col) in enumerate(OFFSETS):
        source = slopes[k] * share
        given[step_col] = given[step_col] + turn(source * supply, -step_row, 0)
        weight[step_row, step_col] = source
    flow = core(supply + given[0] + turn(given[1], -1, 1) + turn(given[-1], 1, 1))
    weight = {at: turn(core(weight[at]), -at[1], 1) for at in weight}
    supply = core(supply)

    def sweep(flow):
        moved = {step: turn(flow, -step, 1) for step in (-1, 0, 1)}
        sums = {}
        for step_row in (-1, 0, 1):
            sums[step_row] = functools.reduce(
                jnp.add, [weight[step_row, c] * moved[c] for c in (-1, 0, 1) if (step_row, c) in weight])
        return supply + sums[0] + turn(sums[1], -1, 0) + turn(sums[-1], 1, 0)

    def beside_line(x, step):
        moved = pltpu.roll(x, 1 if step < 0 else LANES - 1, 1)
        edge = pltpu.roll(moved, 1 if step < 0 else 7, 0)
        return jnp.where(lane == (0 if step < 0 else LANES - 1), edge, moved)

    def around(line):
        return {0: line, -1: beside_line(line, -1), 1: beside_line(line, 1)}

    outermost = jnp.logical_or(jnp.logical_and(sub == 0, lane == 0), jnp.logical_and(sub == far, lane == LANES - 1))
    own_lines = ([32 + 2 * crows, 24 + 2 * crows], [0, 8])
    own_lines = [[around(tall[at:at + 8, :]) for at in pair] for pair in own_lines]

    def edge_row(slot):
        inward, number = (-1, 1) if slot == 0 else (1, 0)
        outside = [around(vrecv[slot, line_at[slot] + 8 * i:line_at[slot] + 8 * i + 8, :]) for i in ((0, 1) if slot == 0 else (1, 0))]
        edge, following = own_lines[slot]

        def given(source, near):
            slopes = {at: coef[k] * jnp.maximum(source[0] - near[at[0]][at[1]], 0.0) for k, at in enumerate(OFFSETS)}
            share = jnp.where(outermost, 0.0, 1.0 / (functools.reduce(jnp.add, slopes.values()) + RETENTION))
            return {at: slopes[at] * share for at in slopes}

        def spread(flux, row_step):
            west, east = beside_line(flux[row_step, 1], -1), beside_line(flux[row_step, -1], 1)
            kept = jnp.where(first, 0.0, west) + jnp.where(last, 0.0, east)
            if row_step != 0:
                kept = kept + flux[row_step, 0]
            return kept, jnp.where(first, west, jnp.where(last, east, 0.0))

        from_outside = given(outside[0], {inward: edge, 0: outside[0], -inward: outside[1]})
        from_edge = given(edge, {inward: following, 0: edge, -inward: outside[0]})
        row_at = 0 if slot == 1 else rows - 1
        for values, refs, at in (
                (spread(from_outside, inward), (inner_edge, outer_edge),
                 pl.ds(number * blocks * groups + (0 if slot == 1 else groups - 1), blocks, stride=groups)),
                (spread(from_edge, 0), (inner, outer), pl.ds(row_at, blocks, stride=rows)),
                (spread(from_edge, inward), (inner, outer), pl.ds(row_at + inward, blocks, stride=rows))):
            for value, ref in zip(values, refs):
                ref[at, :] = ref[at, :] + value

    def column(own, left, right):
        beside = jnp.where(sub < 2, pltpu.roll(left, 4, 0), pltpu.roll(right, 4, 0))
        return jnp.where(jnp.logical_and(sub >= 2, sub < 6), own, beside)

    def edge_columns():
        side_tile = [srecv[k, crows:crows + 8, :] for k in range(8)]
        tall_tile = [vrecv[slot, tile_at[slot]:tile_at[slot] + 8, :] for slot in range(2)]
        tile = tall[16 + 2 * crows:24 + 2 * crows, :]
        below = column(tall_tile[0], side_tile[3], side_tile[1])
        above = column(tall_tile[1], side_tile[5], side_tile[7])
        ze = jnp.concatenate([column(tile, side_tile[4], side_tile[0]), jnp.where(lane < half, below, above)], axis=1)
        sub_e = lax.broadcasted_iota(jnp.int32, (8, 2 * LANES), 0)
        beside_e = {step: turn(ze, step, 1) for step in (-1, 0, 1)}
        flux = {}
        for k, (off_row, off_col) in enumerate(OFFSETS):
            flux[off_row, off_col] = coef[k] * jnp.maximum(ze - turn(beside_e[off_row], off_col, 0), 0.0)
        share_e = 1.0 / (functools.reduce(jnp.add, flux.values()) + RETENTION)

        def lines_of(off_row):
            right, left = flux[off_row, 1] * share_e, flux[off_row, -1] * share_e
            picked = jnp.where(sub_e == 1, right, jnp.where(sub_e == 6, left, 0.0))
            picked = jnp.where(sub_e == 3, pltpu.roll(right, 1, 0), jnp.where(sub_e == 4, pltpu.roll(left, 7, 0), picked))
            if off_row == 0:
                return picked
            return jnp.where(jnp.logical_or(sub_e == 2, sub_e == 5), flux[off_row, 0] * share_e, picked)

        from_above = turn(lines_of(1), -1, 1)[:, :LANES]
        from_below = turn(lines_of(-1), 1, 1)[:, :LANES]
        inside = lines_of(0)[:, :LANES] + jnp.where(first, 0.0, from_above) + jnp.where(last, 0.0, from_below)
        outside = jnp.where(first, from_above, jnp.where(last, from_below, 0.0))
        return inside, outside

    picks = jnp.concatenate([where_lane for where_lane in (
        jnp.where(jnp.logical_or(jnp.logical_and(sub < 4, lane == sub - 2), jnp.logical_and(sub >= 4, lane == sub + (LANES - 6))),
                  jnp.where(jnp.logical_and(sub >= 2, sub < 6), 1.0, 0.0), 0.0),
        jnp.where(jnp.logical_or(jnp.logical_and(sub == 1, lane == 0), jnp.logical_and(sub == 6, lane == LANES - 1)), 1.0, 0.0))], axis=1)
    picks = jnp.concatenate([picks] * 3, axis=0).astype(jnp.bfloat16)

    def upright(lines):
        high = lines.astype(jnp.bfloat16)
        rest = lines - high.astype(F32)
        middle = rest.astype(jnp.bfloat16)
        low = (rest - middle.astype(F32)).astype(jnp.bfloat16)
        split = jnp.concatenate([high.astype(F32), middle.astype(F32), low.astype(F32)], axis=0)
        return jnp.dot(jnp.transpose(split).astype(jnp.bfloat16), picks, preferred_element_type=F32)

    def add_inside(values):
        for field, start in ((inner, 0), (outer, LANES)):
            for g in range(groups):
                value = values[8 * g:8 * g + 8, start:start + LANES]
                for j, chosen in ((0, jnp.where(lane < half, value, 0.0)), (far, jnp.where(lane < half, 0.0, value))):
                    at = pl.ds(j * rows + 8 * g, 8)
                    field[at, :] = field[at, :] + chosen

    def add_outside(values):
        for which, field in enumerate((inner_edge, outer_edge)):
            turned[which] = values[:, which * LANES:(which + 1) * LANES]
            for number in range(2):
                for h in range(halves):
                    value = turned[which, pl.ds(64 * h + 7 * number, 8, stride=8), :]
                    for j, chosen in ((0, jnp.where(lane < half, value, 0.0)), (far, jnp.where(lane < half, 0.0, value))):
                        at = edge_at(number, j, h)
                        field[at, :] = field[at, :] + chosen

    def sent(k):
        @pl.when(exists[k])
        def _():
            copies(k).wait_send()

    flow = sweep(flow)
    sent(0)
    inside, outside = edge_columns()
    flow = sweep(flow)
    edge_row(0)
    flow = sweep(flow)
    sent(1)
    upright_inside, upright_outside = upright(inside), upright(outside)
    flow = sweep(flow)
    edge_row(1)
    flow = sweep(flow)
    flow = sweep(flow)
    sent(2)
    add_inside(upright_inside)
    add_outside(upright_outside)
    flow = sweep(flow)
    for k in range(3, 8):
        sent(k)

    flow_ref[...] = flow


def finish(flow_ref, base, inner, outer, inner_edge, outer_edge, out_ref, result, sem):
    blocks, rows, _ = base.shape
    groups, far = rows // 8, blocks - 1
    halves = groups // 8
    lane = lax.broadcasted_iota(jnp.int32, (8, LANES), 1)
    sub = lax.broadcasted_iota(jnp.int32, (8, LANES), 0)
    first, last = (lane & 7) == 0, (lane & 7) == 7
    per_block = LANES // 8
    aside = jnp.where(first, -1, jnp.where(last, 1, 0))
    flow = [flow_ref[8 * h:8 * h + 8, :] for h in range(halves + 2)]
    beyond = jnp.where(lax.broadcasted_iota(jnp.int32, (8, 2 * LANES), 0) < 4, flow[halves], flow[halves + 1])
    places = [(x[:, :LANES], x[:, LANES:]) for x in flow[:halves] + [beyond]]
    copies = [
        pltpu.make_async_copy(result.at[j], out_ref.at[:, pl.ds(j * LANES, LANES)], sem.at[j]) for j in range(blocks)]
    for j in range(blocks):
        index = lane // 8 + j * per_block
        spread = []
        for centre, other in places:
            beside = take_lanes(centre, jnp.clip(index + aside, 0, LANES - 1))
            if j == 0:
                beside = jnp.where(lane == 0, pltpu.roll(other, 1, 1), beside)
            if j == far:
                beside = jnp.where(lane == LANES - 1, pltpu.roll(other, LANES - 1, 1), beside)
            spread.append((take_lanes(centre, index), beside))
        for g in range(groups):
            def level(number):
                return jnp.broadcast_to(spread[g // 8][number][g % 8:g % 8 + 1, :], (8, LANES))

            at, flat = pl.ds(8 * g, 8), pl.ds(j * rows + 8 * g, 8)
            result[j, at, :] = base[j, at, :] + inner[flat, :] * level(0) + outer[flat, :] * level(1)
        for h in range(halves):
            for number in range(2):
                terms = []
                for which in range(2):
                    here = spread[h][which]
                    if number == 0:
                        other = spread[h - 1][which] if h > 0 else spread[-1][which]
                        level = jnp.where(sub == 0, pltpu.roll(other, 1, 0), pltpu.roll(here, 1, 0))
                    else:
                        other = spread[h + 1][which] if h < halves - 1 else spread[-1][which]
                        level = jnp.where(sub == 7, pltpu.roll(other, 7, 0), pltpu.roll(here, 7, 0))
                    flat = pl.ds((number * blocks + j) * groups + 8 * h, 8)
                    terms.append((inner_edge, outer_edge)[which][flat, :] * level)
                at = pl.ds(64 * h + 7 * number, 8, stride=8)
                result[j, at, :] = result[j, at, :] + (terms[0] + terms[1])
        copies[j].start()
    for copy in copies:
        copy.wait()


def solution(mesh):
    row_devices, col_devices = mesh.shape["rows"], mesh.shape["cols"]

    def on_device(elevation, data_mask, tie_order):
        rows, cols = elevation.shape
        groups, blocks = rows // 8, cols // LANES
        tall = 24 + 2 * groups
        vmem = pl.BlockSpec(memory_space=pltpu.VMEM)
        fields = [
            (2 * groups, 2 * LANES), (blocks, rows, LANES), (blocks * rows, LANES), (blocks * rows, LANES),
            (2 * blocks * groups, LANES), (2 * blocks * groups, LANES)]
        given = pl.pallas_call(
            functools.partial(exchange, row_devices, col_devices),
            out_shape=[pltpu.VMEM(shape, F32) for shape in fields],
            in_specs=[pl.BlockSpec(memory_space=pl.ANY)] * 3,
            out_specs=[vmem] * len(fields),
            scratch_shapes=[
                pltpu.SMEM((8,), jnp.int32),
                pltpu.VMEM((blocks, rows + 16, LANES), F32),
                pltpu.VMEM((blocks, rows + 16, LANES), F32),
                pltpu.VMEM((blocks, rows + 16, LANES), F32),
                pltpu.VMEM((blocks, rows, LANES), jnp.int32),
                pltpu.VMEM((blocks, rows + 16, LANES), F32),
                pltpu.VMEM((2, rows, LANES), F32),
                pltpu.VMEM((cols, 2 * LANES), jnp.bfloat16),
                pltpu.VMEM((4 * groups, cols), jnp.bfloat16),
                pltpu.VMEM((groups + 8, LANES), F32),
                pltpu.VMEM((tall + 16, LANES), F32),
                pltpu.VMEM((8, groups + 8, LANES), F32),
                pltpu.VMEM((2, tall, LANES), F32),
                pltpu.SemaphoreType.DMA((2 * blocks,)),
                pltpu.SemaphoreType.DMA,
                pltpu.SemaphoreType.DMA((8,)),
                pltpu.SemaphoreType.DMA((8,)),
            ],
            compiler_params=pltpu.CompilerParams(collective_id=0, has_side_effects=True, vmem_limit_bytes=61000000),
        )(tie_order, elevation, data_mask)
        return pl.pallas_call(
            finish,
            out_shape=jax.ShapeDtypeStruct((rows, cols), F32),
            in_specs=[vmem] * len(fields),
            out_specs=pl.BlockSpec(memory_space=pl.ANY),
            scratch_shapes=[pltpu.VMEM((blocks, rows, LANES), F32), pltpu.SemaphoreType.DMA((blocks,))],
            compiler_params=pltpu.CompilerParams(vmem_limit_bytes=40000000),
        )(*given)

    return jax.shard_map(
        on_device, mesh=mesh, in_specs=(P("rows", "cols"), P("rows", "cols"), P()),
        out_specs=P("rows", "cols"), check_vma=False)
```

```python
import functools

import jax
import jax.numpy as jnp
from jax import lax
from jax.experimental import pallas as pl
from jax.experimental.pallas import tpu as pltpu
from jax.sharding import PartitionSpec as P

ITERS = 8
OFFSETS = ((0, 1), (1, 1), (1, 0), (1, -1), (0, -1), (-1, -1), (-1, 0), (-1, 1))
RECIPROCAL = (1.0, 0.7071067811865476) * 4
RETENTION = 0.1
OUTSIDE = 1000.0
LANES = 128
F32 = jnp.float32


def coefficients(tie_ref):
    out = []
    for k in range(8):
        value = jnp.float32(0.0)
        for i in range(8):
            place = jnp.float32((1.0 + 0.5 * (7.0 - i) / 7.0) * RECIPROCAL[k])
            value = jnp.where(tie_ref[i] == k, place, value)
        out.append(value)
    return out


def shift_lanes(before, here, after, step, lane):
    if step == 0:
        return here
    if step < 0:
        return pltpu.roll(jnp.where(lane == LANES - 1, before, here), 1, 1)
    return pltpu.roll(jnp.where(lane == 0, after, here), LANES - 1, 1)


def take_lanes(values, index):
    return jnp.take_along_axis(values, index, axis=1, mode="promise_in_bounds")


def exchange(row_devices, col_devices, tie_hbm, elev_ref, mask_ref, flow_ref, base, inner, outer, inner_edge, outer_edge,
             tie_ref, zp, zl, zr, mask, recip, turned, ones, sums, side, tall, srecv, vrecv, load_sem, tie_sem, send_sem, recv_sem):
    rows, cols = elev_ref.shape
    groups, blocks = rows // 8, cols // LANES
    crows, halves = groups, groups // 8
    row, col = lax.axis_index("rows"), lax.axis_index("cols")
    far = blocks - 1

    loads = {}
    for j in [0, far] + list(range(1, far)):
        part = pl.ds(j * LANES, LANES)
        loads[j] = (
            pltpu.make_async_copy(elev_ref.at[:, part], zp.at[j, pl.ds(8, rows), :], load_sem.at[0 if j in (0, far) else 1]),
            pltpu.make_async_copy(mask_ref.at[:, part], mask.at[j], load_sem.at[0 if j in (0, far) else 2]))
    for j in (0, far):
        loads[j][0].start()
        loads[j][1].start()

    barrier = pltpu.get_barrier_semaphore()
    exists = []
    for step_row, step_col in OFFSETS:
        there = jnp.bool_(True)
        if step_row > 0:
            there = row < row_devices - 1
        if step_row < 0:
            there = row > 0
        if step_col > 0:
            there = jnp.logical_and(there, col < col_devices - 1)
        if step_col < 0:
            there = jnp.logical_and(there, col > 0)
        exists.append(there)

    def peer(k):
        return {"rows": row + OFFSETS[k][0], "cols": col + OFFSETS[k][1]}

    for k in (5, 6, 4, 7, 3, 2, 1, 0):
        @pl.when(exists[k])
        def _():
            pl.semaphore_signal(barrier, inc=1, device_id=peer(k), device_id_type=pl.DeviceIdType.MESH)

    for j in range(1, far):
        loads[j][0].start()
        loads[j][1].start()
    tie_load = pltpu.make_async_copy(tie_hbm, tie_ref, tie_sem)
    tie_load.start()

    lane = lax.broadcasted_iota(jnp.int32, (8, LANES), 1)
    sub = lax.broadcasted_iota(jnp.int32, (8, LANES), 0)
    first, last = (lane & 7) == 0, (lane & 7) == 7
    lane_c = lax.broadcasted_iota(jnp.int32, (crows, LANES), 1)
    middle_lanes = jnp.logical_and(lane_c >= LANES // 4, lane_c < 3 * LANES // 4)
    half = LANES // 2
    nothing = jnp.zeros((8, LANES), F32)

    SIDES, UPDOWN = (0, 1, 3, 4, 5, 7), (2, 6)

    taker = lax.broadcasted_iota(jnp.int32, (cols, LANES), 1)
    giver = lax.broadcasted_iota(jnp.int32, (cols, LANES), 0) // 8

    def chosen(here, wanted):
        return (here == wanted).astype(F32).astype(jnp.bfloat16)

    ones[0:cols, :] = chosen(giver, taker)
    for part, start in ((0, 0), (1, far * LANES)):
        ones[cols + part * LANES:cols + (part + 1) * LANES, :] = chosen(giver[start:start + LANES], taker[0:LANES] ^ half)

    order = list(loads)

    def row_sums(some):
        for j in some:
            height_sum = jnp.zeros((crows, LANES), F32)
            count_sum = jnp.zeros((crows, LANES), F32)
            for s in range(8):
                valid = mask[j, pl.ds(s, crows, stride=8), :].astype(F32)
                height_sum = height_sum + valid * zp[j, pl.ds(8 + s, crows, stride=8), :]
                count_sum = count_sum + valid
            high = height_sum.astype(jnp.bfloat16)
            rest = height_sum - high.astype(F32)
            middle = rest.astype(jnp.bfloat16)
            low = (rest - middle.astype(F32)).astype(jnp.bfloat16)
            sums[:, j * LANES:(j + 1) * LANES] = jnp.concatenate([count_sum.astype(jnp.bfloat16), high, middle, low], axis=0)
            for number, at in enumerate((8, 9, rows + 6, rows + 7)):
                line = (0, 8, 24 + 2 * crows, 32 + 2 * crows)[number]
                tall[line + j:line + j + 1, :] = zp[j, at:at + 1, :]

    def loaded(number, count):
        whole = mask.at[pl.ds(0, count)]
        pltpu.make_async_copy(whole, whole, load_sem.at[number]).wait()

    loaded(0, 4)
    ends = jnp.where(lax.broadcasted_iota(jnp.int32, (rows, LANES), 1) < half, zp[0, 8:8 + rows, :], zp[far, 8:8 + rows, :])
    ends = jnp.transpose(ends)
    tile = jnp.where(sub < 4, pltpu.roll(ends[0:8], 2, 0), pltpu.roll(ends[LANES - 8:LANES], 6, 0))
    tall[16 + 2 * crows:24 + 2 * crows, :] = tile
    side[crows:crows + 8, :] = tile
    row_sums((0, far))

    def levels(total):
        counts = total[0:crows]
        heights = total[crows:2 * crows] + (total[2 * crows:3 * crows] + total[3 * crows:])
        return heights / (counts + 1.0), counts * (1.0 / 64.0)

    at_ends = jnp.concatenate([sums[:, 0:LANES], sums[:, far * LANES:]], axis=1)
    from_ends = jnp.concatenate([ones[0:LANES, :], ones[far * LANES:cols, :]], axis=0)
    overview, _ = levels(jnp.dot(at_ends, from_ends, preferred_element_type=F32))
    turned_counts = jnp.dot(at_ends[0:crows], ones[cols:, :], preferred_element_type=F32)
    side[0:crows, :] = jnp.where(middle_lanes, turned_counts * (1.0 / 64.0), overview)

    pl.semaphore_wait(barrier, functools.reduce(jnp.add, [there.astype(jnp.int32) for there in exists]))

    def copies(k, arriving=False):
        slot = k if arriving else (k + 4) % 8
        if k in UPDOWN:
            src, dst = tall.at[pl.ds(16 if k == 2 else 0, 24 + 2 * crows), :], vrecv.at[slot // 4]
        else:
            src, dst = side, srecv.at[slot]
        return pltpu.make_async_remote_copy(
            src_ref=src, dst_ref=dst, send_sem=send_sem.at[k % 4 // 2 if k in UPDOWN else 0], recv_sem=recv_sem,
            device_id=peer(k), device_id_type=pl.DeviceIdType.MESH)

    def send(ks):
        for k in ks:
            @pl.when(exists[k])
            def _():
                copies(k).start()

    send((5, 4, 7, 3, 1, 0))

    for number in (1, 2):
        loaded(number, blocks - 2)
    row_sums(order[2:])
    overview, runoff = levels(jnp.dot(sums[...], ones[0:cols, :], preferred_element_type=F32))
    tall[16:16 + crows, :] = overview
    tall[16 + crows:16 + 2 * crows, :] = runoff

    send((6, 2))

    for k in range(8):
        @pl.when(jnp.logical_not(exists[k]))
        def _():
            if k in UPDOWN:
                for at in range(0, 24 + 2 * crows, 8):
                    start = 16 + crows if k == 2 else crows
                    vrecv[k // 4, at:at + 8, :] = jnp.full((8, LANES), 0.0 if start <= at < start + crows else OUTSIDE, F32)
            else:
                srecv[k, 0:crows, :] = jnp.where(middle_lanes, 0.0, OUTSIDE)
                srecv[k, crows:crows + 8, :] = jnp.full((8, LANES), OUTSIDE, F32)

    tie_load.wait()
    coef = coefficients(tie_ref)

    for ref in (zp, zl, zr, recip):
        for j in range(blocks):
            ref[j, 0:8, :], ref[j, 8 + rows:16 + rows, :] = nothing, nothing

    for g in range(groups):
        at = pl.ds(8 * g + 8, 8)
        for j in range(blocks):
            here = zp[j, at, :]
            before, after = zp[(j - 1) % blocks, at, :], zp[(j + 1) % blocks, at, :]
            zl[j, at, :] = shift_lanes(before, here, after, -1, lane)
            zr[j, at, :] = shift_lanes(before, here, after, 1, lane)
            base[j, pl.ds(8 * g, 8), :] = mask[j, pl.ds(8 * g, 8), :].astype(F32)

    by_column = {-1: zl, 0: zp, 1: zr}

    def within(j, share):
        if j == 0:
            share = jnp.where(lane == 0, 0.0, share)
        if j == far:
            share = jnp.where(lane == LANES - 1, 0.0, share)
        return share

    def leaving(g, j):
        here = zp[j, pl.ds(8 * g + 8, 8), :]
        slopes = {}
        for k, (off_row, off_col) in enumerate(OFFSETS):
            beside = by_column[off_col][j, pl.ds(8 * g + 8 + off_row, 8), :]
            slopes[off_row, off_col] = coef[k] * jnp.maximum(here - beside, 0.0)
        share = within(j, 1.0 / (functools.reduce(jnp.add, slopes.values()) + RETENTION))
        if g == 0:
            share = jnp.where(sub == 0, 0.0, share)
        if g == groups - 1:
            share = jnp.where(sub == 7, 0.0, share)
        recip[j, pl.ds(8 * g + 8, 8), :] = share
        down, up = jnp.where(sub == 7, 0.0, share), jnp.where(sub == 0, 0.0, share)
        out = []
        for c in (-1, 0, 1):
            moved = pltpu.roll(slopes[1, c] * down, 1, 0) + pltpu.roll(slopes[-1, c] * up, 7, 0)
            out.append(moved if c == 0 else moved + slopes[0, c] * share)
        return out

    def across(fields, j):
        west = fields[j - 1][2] if j > 0 else nothing
        east = fields[j + 1][0] if j < far else nothing
        from_west = pltpu.roll(jnp.where(lane == LANES - 1, west, fields[j][2]), 1, 1)
        from_east = pltpu.roll(jnp.where(lane == 0, east, fields[j][0]), LANES - 1, 1)
        kept = fields[j][1] + jnp.where(first, 0.0, from_west) + jnp.where(last, 0.0, from_east)
        return kept, jnp.where(first, from_west, jnp.where(last, from_east, 0.0))

    def settle(g, fields):
        for j in range(blocks):
            at = pl.ds(j * rows + 8 * g, 8)
            inner[at, :], outer[at, :] = across(fields, j)

    for g in range(groups):
        settle(g, [leaving(g, j) for j in range(blocks)])

    def edge_at(number, j, h):
        return pl.ds((number * blocks + j) * groups + 8 * h, 8)

    def compact(number, way, h):
        target = pl.ds(8 + 64 * h + (0 if way == 1 else 7), 8, stride=8)
        source = pl.ds(8 + 64 * h + (-1 if way == 1 else 8), 8, stride=8)
        fields = []
        for j in range(blocks):
            from_z, scale = zp[j, source, :], recip[j, source, :]
            fields.append([
                coef[OFFSETS.index((way, c))] * jnp.maximum(from_z - by_column[c][j, target, :], 0.0) * scale for c in (-1, 0, 1)])
        for j in range(blocks):
            at = edge_at(number, j, h)
            inner_edge[at, :], outer_edge[at, :] = across(fields, j)

    for number, way in enumerate((1, -1)):
        for h in range(halves):
            compact(number, way, h)

    along_rows, along_cols = [
        exists[a].astype(jnp.int32) + exists[b].astype(jnp.int32) for a, b in ((2, 6), (0, 4))]

    def all_of(sem, sides, updown):
        for a in range(min(row_devices - 1, 1), min(row_devices - 1, 2) + 1):
            for b in range(min(col_devices - 1, 1), min(col_devices - 1, 2) + 1):
                lines = sides * (crows + 8) * (b + a * b) + updown * (24 + 2 * crows) * a
                if lines > 0:
                    @pl.when(jnp.logical_and(along_rows == a, along_cols == b))
                    def _():
                        part = turned.at[pl.ds(0, lines), :]
                        pltpu.make_async_copy(part, part, sem).wait()

    all_of(send_sem.at[0], 1, 0)
    all_of(send_sem.at[1], 0, 1)
    all_of(recv_sem, 1, 1)

    def turn(x, step, axis):
        return x if step == 0 else pltpu.roll(x, (-step) % x.shape[axis], axis)

    coarse_at = (16, 0)
    tile_at = (16 + 2 * crows, 2 * crows)
    line_at = (0, 24 + 2 * crows - 16)

    def stacked(of_place):
        end = halves - 1
        rows_of = [of_place(None, h) for h in range(halves)] + [of_place(0, 0)]
        return jnp.concatenate(rows_of + [jnp.where(sub < 4, of_place(0, 1), of_place(1, end - 1)), of_place(1, end)], axis=0)

    def middle_of(field):
        def of_place(slot, h):
            if slot is None:
                return tall[16 + field * crows + 8 * h:24 + field * crows + 8 * h, :]
            return vrecv[slot, coarse_at[slot] + field * crows + 8 * h:coarse_at[slot] + field * crows + 8 * h + 8, :]

        return stacked(of_place)

    def beside_of(east):
        ks = {None: 0 if east else 4, 0: 1 if east else 3, 1: 7 if east else 5}
        return stacked(lambda slot, h: srecv[ks[slot], 8 * h:8 * h + 8, :])

    east, west = beside_of(True), beside_of(False)
    nearer = lax.broadcasted_iota(jnp.int32, east.shape, 1) < half
    z = jnp.concatenate([middle_of(0), jnp.where(nearer, east, west)], axis=1)
    supply = jnp.concatenate([middle_of(1), pltpu.roll(jnp.where(nearer, west, east), half, 1)], axis=1)
    beside_z = {step: turn(z, step, 1) for step in (-1, 0, 1)}
    slopes = []
    for k, (step_row, step_col) in enumerate(OFFSETS):
        slopes.append(coef[k] * jnp.maximum(beside_z[0] - turn(beside_z[step_col], step_row, 0), 0.0))
    share = 1.0 / (functools.reduce(jnp.add, slopes) + RETENTION)

    def core(x):
        return jnp.concatenate([x[0:crows + 8], x[crows + 16:]], axis=0)

    weight = {}
    given = {-1: 0.0, 0: 0.0, 1: 0.0}
    for k, (step_row, step_col) in enumerate(OFFSETS):
        source = slopes[k] * share
        given[step_col] = given[step_col] + turn(source * supply, -step_row, 0)
        weight[step_row, step_col] = source
    flow = core(supply + given[0] + turn(given[1], -1, 1) + turn(given[-1], 1, 1))
    weight = {at: turn(core(weight[at]), -at[1], 1) for at in weight}
    supply = core(supply)

    def sweep(flow):
        moved = {step: turn(flow, -step, 1) for step in (-1, 0, 1)}
        sums = {}
        for step_row in (-1, 0, 1):
            sums[step_row] = functools.reduce(
                jnp.add, [weight[step_row, c] * moved[c] for c in (-1, 0, 1) if (step_row, c) in weight])
        return supply + sums[0] + turn(sums[1], -1, 0) + turn(sums[-1], 1, 0)

    def beside_line(x, step):
        moved = pltpu.roll(x, 1 if step < 0 else LANES - 1, 1)
        edge = pltpu.roll(moved, 1 if step < 0 else 7, 0)
        return jnp.where(lane == (0 if step < 0 else LANES - 1), edge, moved)

    def around(line):
        return {0: line, -1: beside_line(line, -1), 1: beside_line(line, 1)}

    outermost = jnp.logical_or(jnp.logical_and(sub == 0, lane == 0), jnp.logical_and(sub == far, lane == LANES - 1))
    own_lines = ([32 + 2 * crows, 24 + 2 * crows], [0, 8])
    own_lines = [[around(tall[at:at + 8, :]) for at in pair] for pair in own_lines]

    def edge_row(slot):
        inward, number = (-1, 1) if slot == 0 else (1, 0)
        outside = [around(vrecv[slot, line_at[slot] + 8 * i:line_at[slot] + 8 * i + 8, :]) for i in ((0, 1) if slot == 0 else (1, 0))]
        edge, following = own_lines[slot]

        def given(source, near):
            slopes = {at: coef[k] * jnp.maximum(source[0] - near[at[0]][at[1]], 0.0) for k, at in enumerate(OFFSETS)}
            share = jnp.where(outermost, 0.0, 1.0 / (functools.reduce(jnp.add, slopes.values()) + RETENTION))
            return {at: slopes[at] * share for at in slopes}

        def spread(flux, row_step):
            west, east = beside_line(flux[row_step, 1], -1), beside_line(flux[row_step, -1], 1)
            kept = jnp.where(first, 0.0, west) + jnp.where(last, 0.0, east)
            if row_step != 0:
                kept = kept + flux[row_step, 0]
            return kept, jnp.where(first, west, jnp.where(last, east, 0.0))

        from_outside = given(outside[0], {inward: edge, 0: outside[0], -inward: outside[1]})
        from_edge = given(edge, {inward: following, 0: edge, -inward: outside[0]})
        row_at = 0 if slot == 1 else rows - 1
        for values, refs, at in (
                (spread(from_outside, inward), (inner_edge, outer_edge),
                 pl.ds(number * blocks * groups + (0 if slot == 1 else groups - 1), blocks, stride=groups)),
                (spread(from_edge, 0), (inner, outer), pl.ds(row_at, blocks, stride=rows)),
                (spread(from_edge, inward), (inner, outer), pl.ds(row_at + inward, blocks, stride=rows))):
            for value, ref in zip(values, refs):
                ref[at, :] = ref[at, :] + value

    def column(own, left, right):
        beside = jnp.where(sub < 2, pltpu.roll(left, 4, 0), pltpu.roll(right, 4, 0))
        return jnp.where(jnp.logical_and(sub >= 2, sub < 6), own, beside)

    def edge_columns():
        side_tile = [srecv[k, crows:crows + 8, :] for k in range(8)]
        tall_tile = [vrecv[slot, tile_at[slot]:tile_at[slot] + 8, :] for slot in range(2)]
        tile = tall[16 + 2 * crows:24 + 2 * crows, :]
        below = column(tall_tile[0], side_tile[3], side_tile[1])
        above = column(tall_tile[1], side_tile[5], side_tile[7])
        ze = jnp.concatenate([column(tile, side_tile[4], side_tile[0]), jnp.where(lane < half, below, above)], axis=1)
        sub_e = lax.broadcasted_iota(jnp.int32, (8, 2 * LANES), 0)
        beside_e = {step: turn(ze, step, 1) for step in (-1, 0, 1)}
        flux = {}
        for k, (off_row, off_col) in enumerate(OFFSETS):
            flux[off_row, off_col] = coef[k] * jnp.maximum(ze - turn(beside_e[off_row], off_col, 0), 0.0)
        share_e = 1.0 / (functools.reduce(jnp.add, flux.values()) + RETENTION)

        def lines_of(off_row):
            right, left = flux[off_row, 1] * share_e, flux[off_row, -1] * share_e
            picked = jnp.where(sub_e == 1, right, jnp.where(sub_e == 6, left, 0.0))
            picked = jnp.where(sub_e == 3, pltpu.roll(right, 1, 0), jnp.where(sub_e == 4, pltpu.roll(left, 7, 0), picked))
            if off_row == 0:
                return picked
            return jnp.where(jnp.logical_or(sub_e == 2, sub_e == 5), flux[off_row, 0] * share_e, picked)

        from_above = turn(lines_of(1), -1, 1)[:, :LANES]
        from_below = turn(lines_of(-1), 1, 1)[:, :LANES]
        inside = lines_of(0)[:, :LANES] + jnp.where(first, 0.0, from_above) + jnp.where(last, 0.0, from_below)
        outside = jnp.where(first, from_above, jnp.where(last, from_below, 0.0))
        return inside, outside

    picks = jnp.concatenate([where_lane for where_lane in (
        jnp.where(jnp.logical_or(jnp.logical_and(sub < 4, lane == sub - 2), jnp.logical_and(sub >= 4, lane == sub + (LANES - 6))),
                  jnp.where(jnp.logical_and(sub >= 2, sub < 6), 1.0, 0.0), 0.0),
        jnp.where(jnp.logical_or(jnp.logical_and(sub == 1, lane == 0), jnp.logical_and(sub == 6, lane == LANES - 1)), 1.0, 0.0))], axis=1)
    picks = jnp.concatenate([picks] * 3, axis=0).astype(jnp.bfloat16)

    def upright(lines):
        high = lines.astype(jnp.bfloat16)
        rest = lines - high.astype(F32)
        middle = rest.astype(jnp.bfloat16)
        low = (rest - middle.astype(F32)).astype(jnp.bfloat16)
        split = jnp.concatenate([high.astype(F32), middle.astype(F32), low.astype(F32)], axis=0)
        return jnp.dot(jnp.transpose(split).astype(jnp.bfloat16), picks, preferred_element_type=F32)

    def add_inside(values):
        for field, start in ((inner, 0), (outer, LANES)):
            for g in range(groups):
                value = values[8 * g:8 * g + 8, start:start + LANES]
                for j, chosen in ((0, jnp.where(lane < half, value, 0.0)), (far, jnp.where(lane < half, 0.0, value))):
                    at = pl.ds(j * rows + 8 * g, 8)
                    field[at, :] = field[at, :] + chosen

    def add_outside(values):
        for which, field in enumerate((inner_edge, outer_edge)):
            turned[which * rows:(which + 1) * rows, :] = values[:, which * LANES:(which + 1) * LANES]
            for number in range(2):
                for h in range(halves):
                    value = turned[pl.ds(which * rows + 64 * h + 7 * number, 8, stride=8), :]
                    for j, chosen in ((0, jnp.where(lane < half, value, 0.0)), (far, jnp.where(lane < half, 0.0, value))):
                        at = edge_at(number, j, h)
                        field[at, :] = field[at, :] + chosen

    flow = sweep(flow)
    inside, outside = edge_columns()
    flow = sweep(flow)
    edge_row(0)
    flow = sweep(flow)
    upright_inside, upright_outside = upright(inside), upright(outside)
    flow = sweep(flow)
    edge_row(1)
    flow = sweep(flow)
    flow = sweep(flow)
    add_inside(upright_inside)
    add_outside(upright_outside)
    flow = sweep(flow)

    flow_ref[...] = flow


def finish(flow_ref, base, inner, outer, inner_edge, outer_edge, out_ref, result, sem):
    blocks, rows, _ = base.shape
    groups, far = rows // 8, blocks - 1
    halves = groups // 8
    lane = lax.broadcasted_iota(jnp.int32, (8, LANES), 1)
    sub = lax.broadcasted_iota(jnp.int32, (8, LANES), 0)
    first, last = (lane & 7) == 0, (lane & 7) == 7
    per_block = LANES // 8
    aside = jnp.where(first, -1, jnp.where(last, 1, 0))
    flow = [flow_ref[8 * h:8 * h + 8, :] for h in range(halves + 2)]
    beyond = jnp.where(lax.broadcasted_iota(jnp.int32, (8, 2 * LANES), 0) < 4, flow[halves], flow[halves + 1])
    places = [(x[:, :LANES], x[:, LANES:]) for x in flow[:halves] + [beyond]]
    copies = [
        pltpu.make_async_copy(result.at[j], out_ref.at[:, pl.ds(j * LANES, LANES)], sem) for j in range(blocks)]
    for j in range(blocks):
        index = lane // 8 + j * per_block
        spread = []
        for centre, other in places:
            beside = take_lanes(centre, jnp.clip(index + aside, 0, LANES - 1))
            if j == 0:
                beside = jnp.where(lane == 0, pltpu.roll(other, 1, 1), beside)
            if j == far:
                beside = jnp.where(lane == LANES - 1, pltpu.roll(other, LANES - 1, 1), beside)
            spread.append((take_lanes(centre, index), beside))
        for g in range(groups):
            def level(number):
                return jnp.broadcast_to(spread[g // 8][number][g % 8:g % 8 + 1, :], (8, LANES))

            at, flat = pl.ds(8 * g, 8), pl.ds(j * rows + 8 * g, 8)
            result[j, at, :] = base[j, at, :] + inner[flat, :] * level(0) + outer[flat, :] * level(1)
        for h in range(halves):
            for number in range(2):
                terms = []
                for which in range(2):
                    here = spread[h][which]
                    if number == 0:
                        other = spread[h - 1][which] if h > 0 else spread[-1][which]
                        level = jnp.where(sub == 0, pltpu.roll(other, 1, 0), pltpu.roll(here, 1, 0))
                    else:
                        other = spread[h + 1][which] if h < halves - 1 else spread[-1][which]
                        level = jnp.where(sub == 7, pltpu.roll(other, 7, 0), pltpu.roll(here, 7, 0))
                    flat = pl.ds((number * blocks + j) * groups + 8 * h, 8)
                    terms.append((inner_edge, outer_edge)[which][flat, :] * level)
                at = pl.ds(64 * h + 7 * number, 8, stride=8)
                result[j, at, :] = result[j, at, :] + (terms[0] + terms[1])
        copies[j].start()
    pltpu.make_async_copy(result, result, sem).wait()


def solution(mesh):
    row_devices, col_devices = mesh.shape["rows"], mesh.shape["cols"]

    def on_device(elevation, data_mask, tie_order):
        rows, cols = elevation.shape
        groups, blocks = rows // 8, cols // LANES
        tall = 24 + 2 * groups
        vmem = pl.BlockSpec(memory_space=pltpu.VMEM)
        fields = [
            (2 * groups, 2 * LANES), (blocks, rows, LANES), (blocks * rows, LANES), (blocks * rows, LANES),
            (2 * blocks * groups, LANES), (2 * blocks * groups, LANES)]
        given = pl.pallas_call(
            functools.partial(exchange, row_devices, col_devices),
            out_shape=[pltpu.VMEM(shape, F32) for shape in fields],
            in_specs=[pl.BlockSpec(memory_space=pl.ANY)] * 3,
            out_specs=[vmem] * len(fields),
            scratch_shapes=[
                pltpu.SMEM((8,), jnp.int32),
                pltpu.VMEM((blocks, rows + 16, LANES), F32),
                pltpu.VMEM((blocks, rows + 16, LANES), F32),
                pltpu.VMEM((blocks, rows + 16, LANES), F32),
                pltpu.VMEM((blocks, rows, LANES), jnp.int32),
                pltpu.VMEM((blocks, rows + 16, LANES), F32),
                pltpu.VMEM((2 * rows + 16 * groups, LANES), F32),
                pltpu.VMEM((cols + 2 * LANES, LANES), jnp.bfloat16),
                pltpu.VMEM((4 * groups, cols), jnp.bfloat16),
                pltpu.VMEM((groups + 8, LANES), F32),
                pltpu.VMEM((tall + 16, LANES), F32),
                pltpu.VMEM((8, groups + 8, LANES), F32),
                pltpu.VMEM((2, tall, LANES), F32),
                pltpu.SemaphoreType.DMA((3,)),
                pltpu.SemaphoreType.DMA,
                pltpu.SemaphoreType.DMA((2,)),
                pltpu.SemaphoreType.DMA,
            ],
            compiler_params=pltpu.CompilerParams(collective_id=0, has_side_effects=True, vmem_limit_bytes=61000000),
        )(tie_order, elevation, data_mask)
        return pl.pallas_call(
            finish,
            out_shape=jax.ShapeDtypeStruct((rows, cols), F32),
            in_specs=[vmem] * len(fields),
            out_specs=pl.BlockSpec(memory_space=pl.ANY),
            scratch_shapes=[pltpu.VMEM((blocks, rows, LANES), F32), pltpu.SemaphoreType.DMA],
            compiler_params=pltpu.CompilerParams(vmem_limit_bytes=40000000),
        )(*given)

    return jax.shard_map(
        on_device, mesh=mesh, in_specs=(P("rows", "cols"), P("rows", "cols"), P()),
        out_specs=P("rows", "cols"), check_vma=False)
```

```python
import functools

import jax
import jax.numpy as jnp
from jax import lax
from jax.experimental import pallas as pl
from jax.experimental.pallas import tpu as pltpu
from jax.sharding import PartitionSpec as P

ITERS = 8
OFFSETS = ((0, 1), (1, 1), (1, 0), (1, -1), (0, -1), (-1, -1), (-1, 0), (-1, 1))
RECIPROCAL = (1.0, 0.7071067811865476) * 4
RETENTION = 0.1
OUTSIDE = 1000.0
LANES = 128
F32 = jnp.float32


def coefficients(tie_ref):
    out = []
    for k in range(8):
        value = jnp.float32(0.0)
        for i in range(8):
            place = jnp.float32((1.0 + 0.5 * (7.0 - i) / 7.0) * RECIPROCAL[k])
            value = jnp.where(tie_ref[i] == k, place, value)
        out.append(value)
    return out


def shift_lanes(before, here, after, step, lane):
    if step == 0:
        return here
    if step < 0:
        return pltpu.roll(jnp.where(lane == LANES - 1, before, here), 1, 1)
    return pltpu.roll(jnp.where(lane == 0, after, here), LANES - 1, 1)


def take_lanes(values, index):
    return jnp.take_along_axis(values, index, axis=1, mode="promise_in_bounds")


def exchange(row_devices, col_devices, tie_hbm, elev_ref, mask_ref, flow_ref, base, inner, outer, inner_edge, outer_edge,
             tie_ref, zp, zl, zr, mask, recip, turned, ones, sums, side, tall, srecv, vrecv, load_sem, tie_sem, recv_sem):
    rows, cols = elev_ref.shape
    groups, blocks = rows // 8, cols // LANES
    crows, halves = groups, groups // 8
    row, col = lax.axis_index("rows"), lax.axis_index("cols")
    far = blocks - 1

    loads = {}
    for j in [0, far] + list(range(1, far)):
        part = pl.ds(j * LANES, LANES)
        loads[j] = (
            pltpu.make_async_copy(elev_ref.at[:, part], zp.at[j, pl.ds(8, rows), :], load_sem.at[0 if j in (0, far) else 1]),
            pltpu.make_async_copy(mask_ref.at[:, part], mask.at[j], load_sem.at[0 if j in (0, far) else 1]))
    barrier = pltpu.get_barrier_semaphore()
    exists = []
    for step_row, step_col in OFFSETS:
        there = jnp.bool_(True)
        if step_row > 0:
            there = row < row_devices - 1
        if step_row < 0:
            there = row > 0
        if step_col > 0:
            there = jnp.logical_and(there, col < col_devices - 1)
        if step_col < 0:
            there = jnp.logical_and(there, col > 0)
        exists.append(there)

    def peer(k):
        return {"rows": row + OFFSETS[k][0], "cols": col + OFFSETS[k][1]}

    for k in (5, 6, 4, 7, 3, 2, 1, 0):
        @pl.when(exists[k])
        def _():
            pl.semaphore_signal(barrier, inc=1, device_id=peer(k), device_id_type=pl.DeviceIdType.MESH)

    for j in loads:
        loads[j][0].start()
        loads[j][1].start()
    tie_load = pltpu.make_async_copy(tie_hbm, tie_ref, tie_sem)
    tie_load.start()

    lane = lax.broadcasted_iota(jnp.int32, (8, LANES), 1)
    sub = lax.broadcasted_iota(jnp.int32, (8, LANES), 0)
    first, last = (lane & 7) == 0, (lane & 7) == 7
    lane_c = lax.broadcasted_iota(jnp.int32, (crows, LANES), 1)
    middle_lanes = jnp.logical_and(lane_c >= LANES // 4, lane_c < 3 * LANES // 4)
    half = LANES // 2
    nothing = jnp.zeros((8, LANES), F32)

    SIDES, UPDOWN = (0, 1, 3, 4, 5, 7), (2, 6)

    taker = lax.broadcasted_iota(jnp.int32, (cols, LANES), 1)
    giver = lax.broadcasted_iota(jnp.int32, (cols, LANES), 0) // 8

    def chosen(here, wanted):
        return (here == wanted).astype(F32).astype(jnp.bfloat16)

    ones[0:cols, :] = chosen(giver, taker)
    for part, start in ((0, 0), (1, far * LANES)):
        ones[cols + part * LANES:cols + (part + 1) * LANES, :] = chosen(giver[start:start + LANES], taker[0:LANES] ^ half)

    order = list(loads)

    def row_sums(some):
        for j in some:
            height_sum = jnp.zeros((crows, LANES), F32)
            count_sum = jnp.zeros((crows, LANES), F32)
            for s in range(8):
                valid = mask[j, pl.ds(s, crows, stride=8), :].astype(F32)
                height_sum = height_sum + valid * zp[j, pl.ds(8 + s, crows, stride=8), :]
                count_sum = count_sum + valid
            high = height_sum.astype(jnp.bfloat16)
            rest = height_sum - high.astype(F32)
            middle = rest.astype(jnp.bfloat16)
            low = (rest - middle.astype(F32)).astype(jnp.bfloat16)
            sums[:, j * LANES:(j + 1) * LANES] = jnp.concatenate([count_sum.astype(jnp.bfloat16), high, middle, low], axis=0)
            for number, at in enumerate((8, 9, rows + 6, rows + 7)):
                line = (0, 8, 24 + 2 * crows, 32 + 2 * crows)[number]
                tall[line + j:line + j + 1, :] = zp[j, at:at + 1, :]

    def loaded(number, count):
        whole = turned.at[pl.ds(0, count * rows), :]
        pltpu.make_async_copy(whole, whole, load_sem.at[number]).wait()

    tie_load.wait()
    loaded(0, 4)
    ends = jnp.where(lax.broadcasted_iota(jnp.int32, (rows, LANES), 1) < half, zp[0, 8:8 + rows, :], zp[far, 8:8 + rows, :])
    ends = jnp.transpose(ends)
    tile = jnp.where(sub < 4, pltpu.roll(ends[0:8], 2, 0), pltpu.roll(ends[LANES - 8:LANES], 6, 0))
    tall[16 + 2 * crows:24 + 2 * crows, :] = tile
    side[crows:crows + 8, :] = tile
    row_sums((0, far))

    def levels(total):
        counts = total[0:crows]
        heights = total[crows:2 * crows] + (total[2 * crows:3 * crows] + total[3 * crows:])
        return heights / (counts + 1.0), counts * (1.0 / 64.0)

    at_ends = jnp.concatenate([sums[:, 0:LANES], sums[:, far * LANES:]], axis=1)
    from_ends = jnp.concatenate([ones[0:LANES, :], ones[far * LANES:cols, :]], axis=0)
    overview, _ = levels(jnp.dot(at_ends, from_ends, preferred_element_type=F32))
    turned_counts = jnp.dot(at_ends[0:crows], ones[cols:, :], preferred_element_type=F32)
    side[0:crows, :] = jnp.where(middle_lanes, turned_counts * (1.0 / 64.0), overview)

    pl.semaphore_wait(barrier, functools.reduce(jnp.add, [there.astype(jnp.int32) for there in exists]))

    def copies(k, arriving=False):
        slot = k if arriving else (k + 4) % 8
        if k in UPDOWN:
            src, dst = tall.at[pl.ds(16 if k == 2 else 0, 24 + 2 * crows), :], vrecv.at[slot // 4]
        else:
            src, dst = side, srecv.at[slot]
        return pltpu.make_async_remote_copy(
            src_ref=src, dst_ref=dst, send_sem=tie_sem, recv_sem=recv_sem,
            device_id=peer(k), device_id_type=pl.DeviceIdType.MESH)

    def send(ks):
        for k in ks:
            @pl.when(exists[k])
            def _():
                copies(k).start()

    send((5, 4, 7, 3, 1, 0))

    loaded(1, 2 * blocks - 4)
    row_sums(order[2:])
    overview, runoff = levels(jnp.dot(sums[...], ones[0:cols, :], preferred_element_type=F32))
    tall[16:16 + crows, :] = overview
    tall[16 + crows:16 + 2 * crows, :] = runoff

    send((6, 2))

    for k in range(8):
        @pl.when(jnp.logical_not(exists[k]))
        def _():
            if k in UPDOWN:
                for at in range(0, 24 + 2 * crows, 8):
                    start = 16 + crows if k == 2 else crows
                    vrecv[k // 4, at:at + 8, :] = jnp.full((8, LANES), 0.0 if start <= at < start + crows else OUTSIDE, F32)
            else:
                srecv[k, 0:crows, :] = jnp.where(middle_lanes, 0.0, OUTSIDE)
                srecv[k, crows:crows + 8, :] = jnp.full((8, LANES), OUTSIDE, F32)

    coef = coefficients(tie_ref)

    for ref in (zp, zl, zr, recip):
        for j in range(blocks):
            ref[j, 0:8, :], ref[j, 8 + rows:16 + rows, :] = nothing, nothing

    for g in range(groups):
        at = pl.ds(8 * g + 8, 8)
        for j in range(blocks):
            here = zp[j, at, :]
            before, after = zp[(j - 1) % blocks, at, :], zp[(j + 1) % blocks, at, :]
            zl[j, at, :] = shift_lanes(before, here, after, -1, lane)
            zr[j, at, :] = shift_lanes(before, here, after, 1, lane)
            base[j, pl.ds(8 * g, 8), :] = mask[j, pl.ds(8 * g, 8), :].astype(F32)

    by_column = {-1: zl, 0: zp, 1: zr}

    def within(j, share):
        if j == 0:
            share = jnp.where(lane == 0, 0.0, share)
        if j == far:
            share = jnp.where(lane == LANES - 1, 0.0, share)
        return share

    def leaving(g, j):
        here = zp[j, pl.ds(8 * g + 8, 8), :]
        slopes = {}
        for k, (off_row, off_col) in enumerate(OFFSETS):
            beside = by_column[off_col][j, pl.ds(8 * g + 8 + off_row, 8), :]
            slopes[off_row, off_col] = coef[k] * jnp.maximum(here - beside, 0.0)
        share = within(j, 1.0 / (functools.reduce(jnp.add, slopes.values()) + RETENTION))
        if g == 0:
            share = jnp.where(sub == 0, 0.0, share)
        if g == groups - 1:
            share = jnp.where(sub == 7, 0.0, share)
        recip[j, pl.ds(8 * g + 8, 8), :] = share
        down, up = jnp.where(sub == 7, 0.0, share), jnp.where(sub == 0, 0.0, share)
        out = []
        for c in (-1, 0, 1):
            moved = pltpu.roll(slopes[1, c] * down, 1, 0) + pltpu.roll(slopes[-1, c] * up, 7, 0)
            out.append(moved if c == 0 else moved + slopes[0, c] * share)
        return out

    def across(fields, j):
        west = fields[j - 1][2] if j > 0 else nothing
        east = fields[j + 1][0] if j < far else nothing
        from_west = pltpu.roll(jnp.where(lane == LANES - 1, west, fields[j][2]), 1, 1)
        from_east = pltpu.roll(jnp.where(lane == 0, east, fields[j][0]), LANES - 1, 1)
        kept = fields[j][1] + jnp.where(first, 0.0, from_west) + jnp.where(last, 0.0, from_east)
        return kept, jnp.where(first, from_west, jnp.where(last, from_east, 0.0))

    def settle(g, fields):
        for j in range(blocks):
            at = pl.ds(j * rows + 8 * g, 8)
            inner[at, :], outer[at, :] = across(fields, j)

    for g in range(groups):
        settle(g, [leaving(g, j) for j in range(blocks)])

    def edge_at(number, j, h):
        return pl.ds((number * blocks + j) * groups + 8 * h, 8)

    def compact(number, way, h):
        target = pl.ds(8 + 64 * h + (0 if way == 1 else 7), 8, stride=8)
        source = pl.ds(8 + 64 * h + (-1 if way == 1 else 8), 8, stride=8)
        fields = []
        for j in range(blocks):
            from_z, scale = zp[j, source, :], recip[j, source, :]
            fields.append([
                coef[OFFSETS.index((way, c))] * jnp.maximum(from_z - by_column[c][j, target, :], 0.0) * scale for c in (-1, 0, 1)])
        for j in range(blocks):
            at = edge_at(number, j, h)
            inner_edge[at, :], outer_edge[at, :] = across(fields, j)

    for number, way in enumerate((1, -1)):
        for h in range(halves):
            compact(number, way, h)

    along_rows, along_cols = [
        exists[a].astype(jnp.int32) + exists[b].astype(jnp.int32) for a, b in ((2, 6), (0, 4))]

    def all_of(sem):
        for a in range(min(row_devices - 1, 1), min(row_devices - 1, 2) + 1):
            for b in range(min(col_devices - 1, 1), min(col_devices - 1, 2) + 1):
                lines = (crows + 8) * (b + a * b) + (24 + 2 * crows) * a
                if lines > 0:
                    @pl.when(jnp.logical_and(along_rows == a, along_cols == b))
                    def _():
                        part = turned.at[pl.ds(0, lines), :]
                        pltpu.make_async_copy(part, part, sem).wait()

    all_of(tie_sem)
    all_of(recv_sem)

    def turn(x, step, axis):
        return x if step == 0 else pltpu.roll(x, (-step) % x.shape[axis], axis)

    coarse_at = (16, 0)
    tile_at = (16 + 2 * crows, 2 * crows)
    line_at = (0, 24 + 2 * crows - 16)

    def stacked(of_place):
        end = halves - 1
        rows_of = [of_place(None, h) for h in range(halves)] + [of_place(0, 0)]
        return jnp.concatenate(rows_of + [jnp.where(sub < 4, of_place(0, 1), of_place(1, end - 1)), of_place(1, end)], axis=0)

    def middle_of(field):
        def of_place(slot, h):
            if slot is None:
                return tall[16 + field * crows + 8 * h:24 + field * crows + 8 * h, :]
            return vrecv[slot, coarse_at[slot] + field * crows + 8 * h:coarse_at[slot] + field * crows + 8 * h + 8, :]

        return stacked(of_place)

    def beside_of(east):
        ks = {None: 0 if east else 4, 0: 1 if east else 3, 1: 7 if east else 5}
        return stacked(lambda slot, h: srecv[ks[slot], 8 * h:8 * h + 8, :])

    east, west = beside_of(True), beside_of(False)
    nearer = lax.broadcasted_iota(jnp.int32, east.shape, 1) < half
    z = jnp.concatenate([middle_of(0), jnp.where(nearer, east, west)], axis=1)
    supply = jnp.concatenate([middle_of(1), pltpu.roll(jnp.where(nearer, west, east), half, 1)], axis=1)
    beside_z = {step: turn(z, step, 1) for step in (-1, 0, 1)}
    slopes = []
    for k, (step_row, step_col) in enumerate(OFFSETS):
        slopes.append(coef[k] * jnp.maximum(beside_z[0] - turn(beside_z[step_col], step_row, 0), 0.0))
    share = 1.0 / (functools.reduce(jnp.add, slopes) + RETENTION)

    def core(x):
        return jnp.concatenate([x[0:crows + 8], x[crows + 16:]], axis=0)

    weight = {}
    given = {-1: 0.0, 0: 0.0, 1: 0.0}
    for k, (step_row, step_col) in enumerate(OFFSETS):
        source = slopes[k] * share
        given[step_col] = given[step_col] + turn(source * supply, -step_row, 0)
        weight[step_row, step_col] = source
    flow = core(supply + given[0] + turn(given[1], -1, 1) + turn(given[-1], 1, 1))
    weight = {at: turn(core(weight[at]), -at[1], 1) for at in weight}
    supply = core(supply)

    def sweep(flow):
        moved = {step: turn(flow, -step, 1) for step in (-1, 0, 1)}
        sums = {}
        for step_row in (-1, 0, 1):
            sums[step_row] = functools.reduce(
                jnp.add, [weight[step_row, c] * moved[c] for c in (-1, 0, 1) if (step_row, c) in weight])
        return supply + sums[0] + turn(sums[1], -1, 0) + turn(sums[-1], 1, 0)

    def beside_line(x, step):
        moved = pltpu.roll(x, 1 if step < 0 else LANES - 1, 1)
        edge = pltpu.roll(moved, 1 if step < 0 else 7, 0)
        return jnp.where(lane == (0 if step < 0 else LANES - 1), edge, moved)

    def around(line):
        return {0: line, -1: beside_line(line, -1), 1: beside_line(line, 1)}

    outermost = jnp.logical_or(jnp.logical_and(sub == 0, lane == 0), jnp.logical_and(sub == far, lane == LANES - 1))
    own_lines = ([32 + 2 * crows, 24 + 2 * crows], [0, 8])
    own_lines = [[around(tall[at:at + 8, :]) for at in pair] for pair in own_lines]

    def edge_row(slot):
        inward, number = (-1, 1) if slot == 0 else (1, 0)
        outside = [around(vrecv[slot, line_at[slot] + 8 * i:line_at[slot] + 8 * i + 8, :]) for i in ((0, 1) if slot == 0 else (1, 0))]
        edge, following = own_lines[slot]

        def given(source, near):
            slopes = {at: coef[k] * jnp.maximum(source[0] - near[at[0]][at[1]], 0.0) for k, at in enumerate(OFFSETS)}
            share = jnp.where(outermost, 0.0, 1.0 / (functools.reduce(jnp.add, slopes.values()) + RETENTION))
            return {at: slopes[at] * share for at in slopes}

        def spread(flux, row_step):
            west, east = beside_line(flux[row_step, 1], -1), beside_line(flux[row_step, -1], 1)
            kept = jnp.where(first, 0.0, west) + jnp.where(last, 0.0, east)
            if row_step != 0:
                kept = kept + flux[row_step, 0]
            return kept, jnp.where(first, west, jnp.where(last, east, 0.0))

        from_outside = given(outside[0], {inward: edge, 0: outside[0], -inward: outside[1]})
        from_edge = given(edge, {inward: following, 0: edge, -inward: outside[0]})
        row_at = 0 if slot == 1 else rows - 1
        for values, refs, at in (
                (spread(from_outside, inward), (inner_edge, outer_edge),
                 pl.ds(number * blocks * groups + (0 if slot == 1 else groups - 1), blocks, stride=groups)),
                (spread(from_edge, 0), (inner, outer), pl.ds(row_at, blocks, stride=rows)),
                (spread(from_edge, inward), (inner, outer), pl.ds(row_at + inward, blocks, stride=rows))):
            for value, ref in zip(values, refs):
                ref[at, :] = ref[at, :] + value

    def column(own, left, right):
        beside = jnp.where(sub < 2, pltpu.roll(left, 4, 0), pltpu.roll(right, 4, 0))
        return jnp.where(jnp.logical_and(sub >= 2, sub < 6), own, beside)

    def edge_columns():
        side_tile = [srecv[k, crows:crows + 8, :] for k in range(8)]
        tall_tile = [vrecv[slot, tile_at[slot]:tile_at[slot] + 8, :] for slot in range(2)]
        tile = tall[16 + 2 * crows:24 + 2 * crows, :]
        below = column(tall_tile[0], side_tile[3], side_tile[1])
        above = column(tall_tile[1], side_tile[5], side_tile[7])
        ze = jnp.concatenate([column(tile, side_tile[4], side_tile[0]), jnp.where(lane < half, below, above)], axis=1)
        sub_e = lax.broadcasted_iota(jnp.int32, (8, 2 * LANES), 0)
        beside_e = {step: turn(ze, step, 1) for step in (-1, 0, 1)}
        flux = {}
        for k, (off_row, off_col) in enumerate(OFFSETS):
            flux[off_row, off_col] = coef[k] * jnp.maximum(ze - turn(beside_e[off_row], off_col, 0), 0.0)
        share_e = 1.0 / (functools.reduce(jnp.add, flux.values()) + RETENTION)

        def lines_of(off_row):
            right, left = flux[off_row, 1] * share_e, flux[off_row, -1] * share_e
            picked = jnp.where(sub_e == 1, right, jnp.where(sub_e == 6, left, 0.0))
            picked = jnp.where(sub_e == 3, pltpu.roll(right, 1, 0), jnp.where(sub_e == 4, pltpu.roll(left, 7, 0), picked))
            if off_row == 0:
                return picked
            return jnp.where(jnp.logical_or(sub_e == 2, sub_e == 5), flux[off_row, 0] * share_e, picked)

        from_above = turn(lines_of(1), -1, 1)[:, :LANES]
        from_below = turn(lines_of(-1), 1, 1)[:, :LANES]
        inside = lines_of(0)[:, :LANES] + jnp.where(first, 0.0, from_above) + jnp.where(last, 0.0, from_below)
        outside = jnp.where(first, from_above, jnp.where(last, from_below, 0.0))
        return inside, outside

    picks = jnp.concatenate([where_lane for where_lane in (
        jnp.where(jnp.logical_or(jnp.logical_and(sub < 4, lane == sub - 2), jnp.logical_and(sub >= 4, lane == sub + (LANES - 6))),
                  jnp.where(jnp.logical_and(sub >= 2, sub < 6), 1.0, 0.0), 0.0),
        jnp.where(jnp.logical_or(jnp.logical_and(sub == 1, lane == 0), jnp.logical_and(sub == 6, lane == LANES - 1)), 1.0, 0.0))], axis=1)
    picks = jnp.concatenate([picks] * 3, axis=0).astype(jnp.bfloat16)

    def upright(lines):
        high = lines.astype(jnp.bfloat16)
        rest = lines - high.astype(F32)
        middle = rest.astype(jnp.bfloat16)
        low = (rest - middle.astype(F32)).astype(jnp.bfloat16)
        split = jnp.concatenate([high.astype(F32), middle.astype(F32), low.astype(F32)], axis=0)
        return jnp.dot(jnp.transpose(split).astype(jnp.bfloat16), picks, preferred_element_type=F32)

    def add_inside(values):
        for field, start in ((inner, 0), (outer, LANES)):
            for g in range(groups):
                value = values[8 * g:8 * g + 8, start:start + LANES]
                for j, chosen in ((0, jnp.where(lane < half, value, 0.0)), (far, jnp.where(lane < half, 0.0, value))):
                    at = pl.ds(j * rows + 8 * g, 8)
                    field[at, :] = field[at, :] + chosen

    def add_outside(values):
        for which, field in enumerate((inner_edge, outer_edge)):
            turned[which * rows:(which + 1) * rows, :] = values[:, which * LANES:(which + 1) * LANES]
            for number in range(2):
                for h in range(halves):
                    value = turned[pl.ds(which * rows + 64 * h + 7 * number, 8, stride=8), :]
                    for j, chosen in ((0, jnp.where(lane < half, value, 0.0)), (far, jnp.where(lane < half, 0.0, value))):
                        at = edge_at(number, j, h)
                        field[at, :] = field[at, :] + chosen

    flow = sweep(flow)
    inside, outside = edge_columns()
    flow = sweep(flow)
    edge_row(0)
    flow = sweep(flow)
    upright_inside, upright_outside = upright(inside), upright(outside)
    flow = sweep(flow)
    edge_row(1)
    flow = sweep(flow)
    flow = sweep(flow)
    add_inside(upright_inside)
    add_outside(upright_outside)
    flow = sweep(flow)

    flow_ref[...] = flow


def finish(flow_ref, base, inner, outer, inner_edge, outer_edge, out_ref, result, sem):
    blocks, rows, _ = base.shape
    groups, far = rows // 8, blocks - 1
    halves = groups // 8
    lane = lax.broadcasted_iota(jnp.int32, (8, LANES), 1)
    sub = lax.broadcasted_iota(jnp.int32, (8, LANES), 0)
    first, last = (lane & 7) == 0, (lane & 7) == 7
    per_block = LANES // 8
    aside = jnp.where(first, -1, jnp.where(last, 1, 0))
    flow = [flow_ref[8 * h:8 * h + 8, :] for h in range(halves + 2)]
    beyond = jnp.where(lax.broadcasted_iota(jnp.int32, (8, 2 * LANES), 0) < 4, flow[halves], flow[halves + 1])
    places = [(x[:, :LANES], x[:, LANES:]) for x in flow[:halves] + [beyond]]
    copies = [
        pltpu.make_async_copy(result.at[j], out_ref.at[:, pl.ds(j * LANES, LANES)], sem) for j in range(blocks)]
    for j in range(blocks):
        index = lane // 8 + j * per_block
        spread = []
        for centre, other in places:
            beside = take_lanes(centre, jnp.clip(index + aside, 0, LANES - 1))
            if j == 0:
                beside = jnp.where(lane == 0, pltpu.roll(other, 1, 1), beside)
            if j == far:
                beside = jnp.where(lane == LANES - 1, pltpu.roll(other, LANES - 1, 1), beside)
            spread.append((take_lanes(centre, index), beside))
        for g in range(groups):
            def level(number):
                return jnp.broadcast_to(spread[g // 8][number][g % 8:g % 8 + 1, :], (8, LANES))

            at, flat = pl.ds(8 * g, 8), pl.ds(j * rows + 8 * g, 8)
            result[j, at, :] = base[j, at, :] + inner[flat, :] * level(0) + outer[flat, :] * level(1)
        for h in range(halves):
            for number in range(2):
                terms = []
                for which in range(2):
                    here = spread[h][which]
                    if number == 0:
                        other = spread[h - 1][which] if h > 0 else spread[-1][which]
                        level = jnp.where(sub == 0, pltpu.roll(other, 1, 0), pltpu.roll(here, 1, 0))
                    else:
                        other = spread[h + 1][which] if h < halves - 1 else spread[-1][which]
                        level = jnp.where(sub == 7, pltpu.roll(other, 7, 0), pltpu.roll(here, 7, 0))
                    flat = pl.ds((number * blocks + j) * groups + 8 * h, 8)
                    terms.append((inner_edge, outer_edge)[which][flat, :] * level)
                at = pl.ds(64 * h + 7 * number, 8, stride=8)
                result[j, at, :] = result[j, at, :] + (terms[0] + terms[1])
        copies[j].start()
    pltpu.make_async_copy(result, result, sem).wait()


def solution(mesh):
    row_devices, col_devices = mesh.shape["rows"], mesh.shape["cols"]

    def on_device(elevation, data_mask, tie_order):
        rows, cols = elevation.shape
        groups, blocks = rows // 8, cols // LANES
        tall = 24 + 2 * groups
        vmem = pl.BlockSpec(memory_space=pltpu.VMEM)
        fields = [
            (2 * groups, 2 * LANES), (blocks, rows, LANES), (blocks * rows, LANES), (blocks * rows, LANES),
            (2 * blocks * groups, LANES), (2 * blocks * groups, LANES)]
        given = pl.pallas_call(
            functools.partial(exchange, row_devices, col_devices),
            out_shape=[pltpu.VMEM(shape, F32) for shape in fields],
            in_specs=[pl.BlockSpec(memory_space=pl.ANY)] * 3,
            out_specs=[vmem] * len(fields),
            scratch_shapes=[
                pltpu.SMEM((8,), jnp.int32),
                pltpu.VMEM((blocks, rows + 16, LANES), F32),
                pltpu.VMEM((blocks, rows + 16, LANES), F32),
                pltpu.VMEM((blocks, rows + 16, LANES), F32),
                pltpu.VMEM((blocks, rows, LANES), jnp.int32),
                pltpu.VMEM((blocks, rows + 16, LANES), F32),
                pltpu.VMEM((2 * blocks * rows, LANES), F32),
                pltpu.VMEM((cols + 2 * LANES, LANES), jnp.bfloat16),
                pltpu.VMEM((4 * groups, cols), jnp.bfloat16),
                pltpu.VMEM((groups + 8, LANES), F32),
                pltpu.VMEM((tall + 16, LANES), F32),
                pltpu.VMEM((8, groups + 8, LANES), F32),
                pltpu.VMEM((2, tall, LANES), F32),
                pltpu.SemaphoreType.DMA((2,)),
                pltpu.SemaphoreType.DMA,
                pltpu.SemaphoreType.DMA,
            ],
            compiler_params=pltpu.CompilerParams(collective_id=0, has_side_effects=True, vmem_limit_bytes=61000000),
        )(tie_order, elevation, data_mask)
        return pl.pallas_call(
            finish,
            out_shape=jax.ShapeDtypeStruct((rows, cols), F32),
            in_specs=[vmem] * len(fields),
            out_specs=pl.BlockSpec(memory_space=pl.ANY),
            scratch_shapes=[pltpu.VMEM((blocks, rows, LANES), F32), pltpu.SemaphoreType.DMA],
            compiler_params=pltpu.CompilerParams(vmem_limit_bytes=40000000),
        )(*given)

    return jax.shard_map(
        on_device, mesh=mesh, in_specs=(P("rows", "cols"), P("rows", "cols"), P()),
        out_specs=P("rows", "cols"), check_vma=False)
```

```python
import functools

import jax
import jax.numpy as jnp
from jax import lax
from jax.experimental import pallas as pl
from jax.experimental.pallas import tpu as pltpu
from jax.sharding import PartitionSpec as P

ITERS = 8
OFFSETS = ((0, 1), (1, 1), (1, 0), (1, -1), (0, -1), (-1, -1), (-1, 0), (-1, 1))
RECIPROCAL = (1.0, 0.7071067811865476) * 4
RETENTION = 0.1
OUTSIDE = 1000.0
LANES = 128
F32 = jnp.float32


def coefficients(tie_ref):
    out = []
    for k in range(8):
        value = jnp.float32(0.0)
        for i in range(8):
            place = jnp.float32((1.0 + 0.5 * (7.0 - i) / 7.0) * RECIPROCAL[k])
            value = jnp.where(tie_ref[i] == k, place, value)
        out.append(value)
    return out


def shift_lanes(before, here, after, step, lane):
    if step == 0:
        return here
    if step < 0:
        return pltpu.roll(jnp.where(lane == LANES - 1, before, here), 1, 1)
    return pltpu.roll(jnp.where(lane == 0, after, here), LANES - 1, 1)


def take_lanes(values, index):
    return jnp.take_along_axis(values, index, axis=1, mode="promise_in_bounds")


def exchange(row_devices, col_devices, tie_hbm, elev_ref, mask_ref, flow_ref, base, inner, outer, inner_edge, outer_edge,
             tie_ref, zp, zl, zr, mask, recip, turned, ones, sums, side, tall, srecv, vrecv, load_sem, tie_sem, recv_sem):
    rows, cols = elev_ref.shape
    groups, blocks = rows // 8, cols // LANES
    crows, halves = groups, groups // 8
    row, col = lax.axis_index("rows"), lax.axis_index("cols")
    far = blocks - 1

    loads = {}
    for j in [0, far] + list(range(1, far)):
        part = pl.ds(j * LANES, LANES)
        loads[j] = (
            pltpu.make_async_copy(elev_ref.at[:, part], zp.at[j, pl.ds(8, rows), :], load_sem.at[0 if j in (0, far) else 1]),
            pltpu.make_async_copy(mask_ref.at[:, part], mask.at[j], load_sem.at[0 if j in (0, far) else 1]))
    barrier = pltpu.get_barrier_semaphore()
    exists = []
    for step_row, step_col in OFFSETS:
        there = jnp.bool_(True)
        if step_row > 0:
            there = row < row_devices - 1
        if step_row < 0:
            there = row > 0
        if step_col > 0:
            there = jnp.logical_and(there, col < col_devices - 1)
        if step_col < 0:
            there = jnp.logical_and(there, col > 0)
        exists.append(there)

    def peer(k):
        return {"rows": row + OFFSETS[k][0], "cols": col + OFFSETS[k][1]}

    for k in (5, 6, 4, 7, 3, 2, 1, 0):
        @pl.when(exists[k])
        def _():
            pl.semaphore_signal(barrier, inc=1, device_id=peer(k), device_id_type=pl.DeviceIdType.MESH)

    for j in loads:
        loads[j][0].start()
        loads[j][1].start()
    tie_load = pltpu.make_async_copy(tie_hbm, tie_ref, tie_sem)
    tie_load.start()

    lane = lax.broadcasted_iota(jnp.int32, (8, LANES), 1)
    sub = lax.broadcasted_iota(jnp.int32, (8, LANES), 0)
    first, last = (lane & 7) == 0, (lane & 7) == 7
    lane_c = lax.broadcasted_iota(jnp.int32, (crows, LANES), 1)
    middle_lanes = jnp.logical_and(lane_c >= LANES // 4, lane_c < 3 * LANES // 4)
    half = LANES // 2
    nothing = jnp.zeros((8, LANES), F32)

    SIDES, UPDOWN = (0, 1, 3, 4, 5, 7), (2, 6)

    taker = lax.broadcasted_iota(jnp.int32, (cols, LANES), 1)
    giver = lax.broadcasted_iota(jnp.int32, (cols, LANES), 0) // 8

    def chosen(here, wanted):
        return (here == wanted).astype(F32).astype(jnp.bfloat16)

    ones[0:cols, :] = chosen(giver, taker)
    for part, start in ((0, 0), (1, far * LANES)):
        ones[cols + part * LANES:cols + (part + 1) * LANES, :] = chosen(giver[start:start + LANES], taker[0:LANES] ^ half)

    order = list(loads)

    def turn(x, step, axis):
        return x if step == 0 else pltpu.roll(x, (-step) % x.shape[axis], axis)

    def row_sums(some):
        for j in some:
            height_sum = jnp.zeros((crows, LANES), F32)
            count_sum = jnp.zeros((crows, LANES), F32)
            for s in range(8):
                valid = mask[j, pl.ds(s, crows, stride=8), :].astype(F32)
                height_sum = height_sum + valid * zp[j, pl.ds(8 + s, crows, stride=8), :]
                count_sum = count_sum + valid
            high = height_sum.astype(jnp.bfloat16)
            rest = height_sum - high.astype(F32)
            middle = rest.astype(jnp.bfloat16)
            low = (rest - middle.astype(F32)).astype(jnp.bfloat16)
            sums[:, j * LANES:(j + 1) * LANES] = jnp.concatenate([count_sum.astype(jnp.bfloat16), high, middle, low], axis=0)
            for number, at in enumerate((8, 9, rows + 6, rows + 7)):
                line = (0, 8, 24 + 2 * crows, 32 + 2 * crows)[number]
                tall[line + j:line + j + 1, :] = zp[j, at:at + 1, :]

    def loaded(number, count):
        whole = turned.at[pl.ds(0, count * rows), :]
        pltpu.make_async_copy(whole, whole, load_sem.at[number]).wait()

    tie_load.wait()
    loaded(0, 4)
    ends = jnp.where(lax.broadcasted_iota(jnp.int32, (rows, LANES), 1) < half, zp[0, 8:8 + rows, :], zp[far, 8:8 + rows, :])
    ends = jnp.transpose(ends)
    tile = jnp.where(sub < 4, pltpu.roll(ends[0:8], 2, 0), pltpu.roll(ends[LANES - 8:LANES], 6, 0))
    tall[16 + 2 * crows:24 + 2 * crows, :] = tile
    parts = [turn(tile, 32 * c - 16, 1) for c in range(4)]

    def packed(at):
        value = nothing
        for c in range(4):
            value = jnp.where(sub == c, pltpu.roll(parts[c], (c - at) % 8, 0), value)
            value = jnp.where(sub == c + 4, pltpu.roll(parts[c], (c + 3 - at) % 8, 0), value)
        return value

    lines = jnp.concatenate([packed(2), packed(4)], axis=0)
    row_sums((0, far))

    def levels(total):
        counts = total[0:crows]
        heights = total[crows:2 * crows] + (total[2 * crows:3 * crows] + total[3 * crows:])
        return heights / (counts + 1.0), counts * (1.0 / 64.0)

    at_ends = jnp.concatenate([sums[:, 0:LANES], sums[:, far * LANES:]], axis=1)
    from_ends = jnp.concatenate([ones[0:LANES, :], ones[far * LANES:cols, :]], axis=0)
    overview, _ = levels(jnp.dot(at_ends, from_ends, preferred_element_type=F32))
    turned_counts = jnp.dot(at_ends[0:crows], ones[cols:, :], preferred_element_type=F32)
    side[...] = jnp.where(
        jnp.logical_and(lane_c >= 16, lane_c < 48), lines, jnp.where(middle_lanes, turned_counts * (1.0 / 64.0), overview))

    pl.semaphore_wait(barrier, functools.reduce(jnp.add, [there.astype(jnp.int32) for there in exists]))

    def copies(k, arriving=False):
        slot = k if arriving else (k + 4) % 8
        if k in UPDOWN:
            src, dst = tall.at[pl.ds(16 if k == 2 else 0, 24 + 2 * crows), :], vrecv.at[slot // 4]
        else:
            src, dst = side, srecv.at[slot]
        return pltpu.make_async_remote_copy(
            src_ref=src, dst_ref=dst, send_sem=tie_sem, recv_sem=recv_sem,
            device_id=peer(k), device_id_type=pl.DeviceIdType.MESH)

    def send(ks):
        for k in ks:
            @pl.when(exists[k])
            def _():
                copies(k).start()

    send((5, 4, 7, 3, 1, 0))

    loaded(1, 2 * blocks - 4)
    row_sums(order[2:])
    overview, runoff = levels(jnp.dot(sums[...], ones[0:cols, :], preferred_element_type=F32))
    tall[16:16 + crows, :] = overview
    tall[16 + crows:16 + 2 * crows, :] = runoff

    send((6, 2))

    for k in range(8):
        @pl.when(jnp.logical_not(exists[k]))
        def _():
            if k in UPDOWN:
                for at in range(0, 24 + 2 * crows, 8):
                    start = 16 + crows if k == 2 else crows
                    vrecv[k // 4, at:at + 8, :] = jnp.full((8, LANES), 0.0 if start <= at < start + crows else OUTSIDE, F32)
            else:
                srecv[k] = jnp.where(jnp.logical_and(lane_c >= 48, lane_c < half + 16), 0.0, OUTSIDE)

    coef = coefficients(tie_ref)

    for ref in (zp, zl, zr, recip):
        for j in range(blocks):
            ref[j, 0:8, :], ref[j, 8 + rows:16 + rows, :] = nothing, nothing

    for g in range(groups):
        at = pl.ds(8 * g + 8, 8)
        for j in range(blocks):
            here = zp[j, at, :]
            before, after = zp[(j - 1) % blocks, at, :], zp[(j + 1) % blocks, at, :]
            zl[j, at, :] = shift_lanes(before, here, after, -1, lane)
            zr[j, at, :] = shift_lanes(before, here, after, 1, lane)
            base[j, pl.ds(8 * g, 8), :] = mask[j, pl.ds(8 * g, 8), :].astype(F32)

    by_column = {-1: zl, 0: zp, 1: zr}

    def within(j, share):
        if j == 0:
            share = jnp.where(lane == 0, 0.0, share)
        if j == far:
            share = jnp.where(lane == LANES - 1, 0.0, share)
        return share

    def leaving(g, j):
        here = zp[j, pl.ds(8 * g + 8, 8), :]
        slopes = {}
        for k, (off_row, off_col) in enumerate(OFFSETS):
            beside = by_column[off_col][j, pl.ds(8 * g + 8 + off_row, 8), :]
            slopes[off_row, off_col] = coef[k] * jnp.maximum(here - beside, 0.0)
        share = within(j, 1.0 / (functools.reduce(jnp.add, slopes.values()) + RETENTION))
        if g == 0:
            share = jnp.where(sub == 0, 0.0, share)
        if g == groups - 1:
            share = jnp.where(sub == 7, 0.0, share)
        recip[j, pl.ds(8 * g + 8, 8), :] = share
        down, up = jnp.where(sub == 7, 0.0, share), jnp.where(sub == 0, 0.0, share)
        out = []
        for c in (-1, 0, 1):
            moved = pltpu.roll(slopes[1, c] * down, 1, 0) + pltpu.roll(slopes[-1, c] * up, 7, 0)
            out.append(moved if c == 0 else moved + slopes[0, c] * share)
        return out

    def across(fields, j):
        west = fields[j - 1][2] if j > 0 else nothing
        east = fields[j + 1][0] if j < far else nothing
        from_west = pltpu.roll(jnp.where(lane == LANES - 1, west, fields[j][2]), 1, 1)
        from_east = pltpu.roll(jnp.where(lane == 0, east, fields[j][0]), LANES - 1, 1)
        kept = fields[j][1] + jnp.where(first, 0.0, from_west) + jnp.where(last, 0.0, from_east)
        return kept, jnp.where(first, from_west, jnp.where(last, from_east, 0.0))

    def settle(g, fields):
        for j in range(blocks):
            at = pl.ds(j * rows + 8 * g, 8)
            inner[at, :], outer[at, :] = across(fields, j)

    for g in range(groups):
        settle(g, [leaving(g, j) for j in range(blocks)])

    def edge_at(number, j, h):
        return pl.ds((number * blocks + j) * groups + 8 * h, 8)

    def compact(number, way, h):
        target = pl.ds(8 + 64 * h + (0 if way == 1 else 7), 8, stride=8)
        source = pl.ds(8 + 64 * h + (-1 if way == 1 else 8), 8, stride=8)
        fields = []
        for j in range(blocks):
            from_z, scale = zp[j, source, :], recip[j, source, :]
            fields.append([
                coef[OFFSETS.index((way, c))] * jnp.maximum(from_z - by_column[c][j, target, :], 0.0) * scale for c in (-1, 0, 1)])
        for j in range(blocks):
            at = edge_at(number, j, h)
            inner_edge[at, :], outer_edge[at, :] = across(fields, j)

    for number, way in enumerate((1, -1)):
        for h in range(halves):
            compact(number, way, h)

    along_rows, along_cols = [
        exists[a].astype(jnp.int32) + exists[b].astype(jnp.int32) for a, b in ((2, 6), (0, 4))]

    def all_of(sem):
        for a in range(min(row_devices - 1, 1), min(row_devices - 1, 2) + 1):
            for b in range(min(col_devices - 1, 1), min(col_devices - 1, 2) + 1):
                lines = crows * (b + a * b) + (24 + 2 * crows) * a
                if lines > 0:
                    @pl.when(jnp.logical_and(along_rows == a, along_cols == b))
                    def _():
                        part = turned.at[pl.ds(0, lines), :]
                        pltpu.make_async_copy(part, part, sem).wait()

    all_of(tie_sem)
    all_of(recv_sem)

    coarse_at = (16, 0)
    tile_at = (16 + 2 * crows, 2 * crows)
    line_at = (0, 24 + 2 * crows - 16)

    def stacked(of_place):
        end = halves - 1
        rows_of = [of_place(None, h) for h in range(halves)] + [of_place(0, 0)]
        return jnp.concatenate(rows_of + [jnp.where(sub < 4, of_place(0, 1), of_place(1, end - 1)), of_place(1, end)], axis=0)

    def middle_of(field):
        def of_place(slot, h):
            if slot is None:
                return tall[16 + field * crows + 8 * h:24 + field * crows + 8 * h, :]
            return vrecv[slot, coarse_at[slot] + field * crows + 8 * h:coarse_at[slot] + field * crows + 8 * h + 8, :]

        return stacked(of_place)

    def beside_of(east):
        ks = {None: 0 if east else 4, 0: 1 if east else 3, 1: 7 if east else 5}
        return stacked(lambda slot, h: srecv[ks[slot], 8 * h:8 * h + 8, :])

    east, west = beside_of(True), beside_of(False)
    nearer = lax.broadcasted_iota(jnp.int32, east.shape, 1) < half
    z = jnp.concatenate([middle_of(0), jnp.where(nearer, east, west)], axis=1)
    supply = jnp.concatenate([middle_of(1), pltpu.roll(jnp.where(nearer, west, east), half, 1)], axis=1)
    beside_z = {step: turn(z, step, 1) for step in (-1, 0, 1)}
    slopes = []
    for k, (step_row, step_col) in enumerate(OFFSETS):
        slopes.append(coef[k] * jnp.maximum(beside_z[0] - turn(beside_z[step_col], step_row, 0), 0.0))
    share = 1.0 / (functools.reduce(jnp.add, slopes) + RETENTION)

    def core(x):
        return jnp.concatenate([x[0:crows + 8], x[crows + 16:]], axis=0)

    weight = {}
    given = {-1: 0.0, 0: 0.0, 1: 0.0}
    for k, (step_row, step_col) in enumerate(OFFSETS):
        source = slopes[k] * share
        given[step_col] = given[step_col] + turn(source * supply, -step_row, 0)
        weight[step_row, step_col] = source
    flow = core(supply + given[0] + turn(given[1], -1, 1) + turn(given[-1], 1, 1))
    weight = {at: turn(core(weight[at]), -at[1], 1) for at in weight}
    supply = core(supply)

    def sweep(flow):
        moved = {step: turn(flow, -step, 1) for step in (-1, 0, 1)}
        sums = {}
        for step_row in (-1, 0, 1):
            sums[step_row] = functools.reduce(
                jnp.add, [weight[step_row, c] * moved[c] for c in (-1, 0, 1) if (step_row, c) in weight])
        return supply + sums[0] + turn(sums[1], -1, 0) + turn(sums[-1], 1, 0)

    def beside_line(x, step):
        moved = pltpu.roll(x, 1 if step < 0 else LANES - 1, 1)
        edge = pltpu.roll(moved, 1 if step < 0 else 7, 0)
        return jnp.where(lane == (0 if step < 0 else LANES - 1), edge, moved)

    def around(line):
        return {0: line, -1: beside_line(line, -1), 1: beside_line(line, 1)}

    outermost = jnp.logical_or(jnp.logical_and(sub == 0, lane == 0), jnp.logical_and(sub == far, lane == LANES - 1))
    own_lines = ([32 + 2 * crows, 24 + 2 * crows], [0, 8])
    own_lines = [[around(tall[at:at + 8, :]) for at in pair] for pair in own_lines]

    def edge_row(slot):
        inward, number = (-1, 1) if slot == 0 else (1, 0)
        outside = [around(vrecv[slot, line_at[slot] + 8 * i:line_at[slot] + 8 * i + 8, :]) for i in ((0, 1) if slot == 0 else (1, 0))]
        edge, following = own_lines[slot]

        def given(source, near):
            slopes = {at: coef[k] * jnp.maximum(source[0] - near[at[0]][at[1]], 0.0) for k, at in enumerate(OFFSETS)}
            share = jnp.where(outermost, 0.0, 1.0 / (functools.reduce(jnp.add, slopes.values()) + RETENTION))
            return {at: slopes[at] * share for at in slopes}

        def spread(flux, row_step):
            west, east = beside_line(flux[row_step, 1], -1), beside_line(flux[row_step, -1], 1)
            kept = jnp.where(first, 0.0, west) + jnp.where(last, 0.0, east)
            if row_step != 0:
                kept = kept + flux[row_step, 0]
            return kept, jnp.where(first, west, jnp.where(last, east, 0.0))

        from_outside = given(outside[0], {inward: edge, 0: outside[0], -inward: outside[1]})
        from_edge = given(edge, {inward: following, 0: edge, -inward: outside[0]})
        row_at = 0 if slot == 1 else rows - 1
        for values, refs, at in (
                (spread(from_outside, inward), (inner_edge, outer_edge),
                 pl.ds(number * blocks * groups + (0 if slot == 1 else groups - 1), blocks, stride=groups)),
                (spread(from_edge, 0), (inner, outer), pl.ds(row_at, blocks, stride=rows)),
                (spread(from_edge, inward), (inner, outer), pl.ds(row_at + inward, blocks, stride=rows))):
            for value, ref in zip(values, refs):
                ref[at, :] = ref[at, :] + value

    def column(own, left, right):
        beside = jnp.where(sub < 2, pltpu.roll(left, 4, 0), pltpu.roll(right, 4, 0))
        return jnp.where(jnp.logical_and(sub >= 2, sub < 6), own, beside)

    def edge_columns():
        def unpacked(k):
            start = 2 if OFFSETS[k][1] > 0 else 4
            given = srecv[k, 0:8, :] if OFFSETS[k][1] > 0 else srecv[k, 8:16, :]
            value = nothing
            for c in range(4):
                moved = turn(given, 16 - 32 * c, 1)
                pair = jnp.where(sub == start, pltpu.roll(moved, (start - c) % 8, 0), pltpu.roll(moved, (start - 3 - c) % 8, 0))
                value = jnp.where(lane // 32 == c, pair, value)
            return value

        side_tile = {k: unpacked(k) for k in SIDES}
        tall_tile = [vrecv[slot, tile_at[slot]:tile_at[slot] + 8, :] for slot in range(2)]
        tile = tall[16 + 2 * crows:24 + 2 * crows, :]
        below = column(tall_tile[0], side_tile[3], side_tile[1])
        above = column(tall_tile[1], side_tile[5], side_tile[7])
        ze = jnp.concatenate([column(tile, side_tile[4], side_tile[0]), jnp.where(lane < half, below, above)], axis=1)
        sub_e = lax.broadcasted_iota(jnp.int32, (8, 2 * LANES), 0)
        beside_e = {step: turn(ze, step, 1) for step in (-1, 0, 1)}
        flux = {}
        for k, (off_row, off_col) in enumerate(OFFSETS):
            flux[off_row, off_col] = coef[k] * jnp.maximum(ze - turn(beside_e[off_row], off_col, 0), 0.0)
        share_e = 1.0 / (functools.reduce(jnp.add, flux.values()) + RETENTION)

        def lines_of(off_row):
            right, left = flux[off_row, 1] * share_e, flux[off_row, -1] * share_e
            picked = jnp.where(sub_e == 1, right, jnp.where(sub_e == 6, left, 0.0))
            picked = jnp.where(sub_e == 3, pltpu.roll(right, 1, 0), jnp.where(sub_e == 4, pltpu.roll(left, 7, 0), picked))
            if off_row == 0:
                return picked
            return jnp.where(jnp.logical_or(sub_e == 2, sub_e == 5), flux[off_row, 0] * share_e, picked)

        from_above = turn(lines_of(1), -1, 1)[:, :LANES]
        from_below = turn(lines_of(-1), 1, 1)[:, :LANES]
        inside = lines_of(0)[:, :LANES] + jnp.where(first, 0.0, from_above) + jnp.where(last, 0.0, from_below)
        outside = jnp.where(first, from_above, jnp.where(last, from_below, 0.0))
        return inside, outside

    picks = jnp.concatenate([where_lane for where_lane in (
        jnp.where(jnp.logical_or(jnp.logical_and(sub < 4, lane == sub - 2), jnp.logical_and(sub >= 4, lane == sub + (LANES - 6))),
                  jnp.where(jnp.logical_and(sub >= 2, sub < 6), 1.0, 0.0), 0.0),
        jnp.where(jnp.logical_or(jnp.logical_and(sub == 1, lane == 0), jnp.logical_and(sub == 6, lane == LANES - 1)), 1.0, 0.0))], axis=1)
    picks = jnp.concatenate([picks] * 3, axis=0).astype(jnp.bfloat16)

    def upright(lines):
        high = lines.astype(jnp.bfloat16)
        rest = lines - high.astype(F32)
        middle = rest.astype(jnp.bfloat16)
        low = (rest - middle.astype(F32)).astype(jnp.bfloat16)
        split = jnp.concatenate([high.astype(F32), middle.astype(F32), low.astype(F32)], axis=0)
        return jnp.dot(jnp.transpose(split).astype(jnp.bfloat16), picks, preferred_element_type=F32)

    def add_inside(values):
        for field, start in ((inner, 0), (outer, LANES)):
            for g in range(groups):
                value = values[8 * g:8 * g + 8, start:start + LANES]
                for j, chosen in ((0, jnp.where(lane < half, value, 0.0)), (far, jnp.where(lane < half, 0.0, value))):
                    at = pl.ds(j * rows + 8 * g, 8)
                    field[at, :] = field[at, :] + chosen

    def add_outside(values):
        for which, field in enumerate((inner_edge, outer_edge)):
            turned[which * rows:(which + 1) * rows, :] = values[:, which * LANES:(which + 1) * LANES]
            for number in range(2):
                for h in range(halves):
                    value = turned[pl.ds(which * rows + 64 * h + 7 * number, 8, stride=8), :]
                    for j, chosen in ((0, jnp.where(lane < half, value, 0.0)), (far, jnp.where(lane < half, 0.0, value))):
                        at = edge_at(number, j, h)
                        field[at, :] = field[at, :] + chosen

    flow = sweep(flow)
    inside, outside = edge_columns()
    flow = sweep(flow)
    edge_row(0)
    flow = sweep(flow)
    upright_inside, upright_outside = upright(inside), upright(outside)
    flow = sweep(flow)
    edge_row(1)
    flow = sweep(flow)
    flow = sweep(flow)
    add_inside(upright_inside)
    add_outside(upright_outside)
    flow = sweep(flow)

    flow_ref[...] = flow


def finish(flow_ref, base, inner, outer, inner_edge, outer_edge, out_ref, result, sem):
    blocks, rows, _ = base.shape
    groups, far = rows // 8, blocks - 1
    halves = groups // 8
    lane = lax.broadcasted_iota(jnp.int32, (8, LANES), 1)
    sub = lax.broadcasted_iota(jnp.int32, (8, LANES), 0)
    first, last = (lane & 7) == 0, (lane & 7) == 7
    per_block = LANES // 8
    aside = jnp.where(first, -1, jnp.where(last, 1, 0))
    flow = [flow_ref[8 * h:8 * h + 8, :] for h in range(halves + 2)]
    beyond = jnp.where(lax.broadcasted_iota(jnp.int32, (8, 2 * LANES), 0) < 4, flow[halves], flow[halves + 1])
    places = [(x[:, :LANES], x[:, LANES:]) for x in flow[:halves] + [beyond]]
    copies = [
        pltpu.make_async_copy(result.at[j], out_ref.at[:, pl.ds(j * LANES, LANES)], sem) for j in range(blocks)]
    for j in range(blocks):
        index = lane // 8 + j * per_block
        spread = []
        for centre, other in places:
            beside = take_lanes(centre, jnp.clip(index + aside, 0, LANES - 1))
            if j == 0:
                beside = jnp.where(lane == 0, pltpu.roll(other, 1, 1), beside)
            if j == far:
                beside = jnp.where(lane == LANES - 1, pltpu.roll(other, LANES - 1, 1), beside)
            spread.append((take_lanes(centre, index), beside))
        for g in range(groups):
            def level(number):
                return jnp.broadcast_to(spread[g // 8][number][g % 8:g % 8 + 1, :], (8, LANES))

            at, flat = pl.ds(8 * g, 8), pl.ds(j * rows + 8 * g, 8)
            result[j, at, :] = base[j, at, :] + inner[flat, :] * level(0) + outer[flat, :] * level(1)
        for h in range(halves):
            for number in range(2):
                terms = []
                for which in range(2):
                    here = spread[h][which]
                    if number == 0:
                        other = spread[h - 1][which] if h > 0 else spread[-1][which]
                        level = jnp.where(sub == 0, pltpu.roll(other, 1, 0), pltpu.roll(here, 1, 0))
                    else:
                        other = spread[h + 1][which] if h < halves - 1 else spread[-1][which]
                        level = jnp.where(sub == 7, pltpu.roll(other, 7, 0), pltpu.roll(here, 7, 0))
                    flat = pl.ds((number * blocks + j) * groups + 8 * h, 8)
                    terms.append((inner_edge, outer_edge)[which][flat, :] * level)
                at = pl.ds(64 * h + 7 * number, 8, stride=8)
                result[j, at, :] = result[j, at, :] + (terms[0] + terms[1])
        copies[j].start()
    pltpu.make_async_copy(result, result, sem).wait()


def solution(mesh):
    row_devices, col_devices = mesh.shape["rows"], mesh.shape["cols"]

    def on_device(elevation, data_mask, tie_order):
        rows, cols = elevation.shape
        groups, blocks = rows // 8, cols // LANES
        tall = 24 + 2 * groups
        vmem = pl.BlockSpec(memory_space=pltpu.VMEM)
        fields = [
            (2 * groups, 2 * LANES), (blocks, rows, LANES), (blocks * rows, LANES), (blocks * rows, LANES),
            (2 * blocks * groups, LANES), (2 * blocks * groups, LANES)]
        given = pl.pallas_call(
            functools.partial(exchange, row_devices, col_devices),
            out_shape=[pltpu.VMEM(shape, F32) for shape in fields],
            in_specs=[pl.BlockSpec(memory_space=pl.ANY)] * 3,
            out_specs=[vmem] * len(fields),
            scratch_shapes=[
                pltpu.SMEM((8,), jnp.int32),
                pltpu.VMEM((blocks, rows + 16, LANES), F32),
                pltpu.VMEM((blocks, rows + 16, LANES), F32),
                pltpu.VMEM((blocks, rows + 16, LANES), F32),
                pltpu.VMEM((blocks, rows, LANES), jnp.int32),
                pltpu.VMEM((blocks, rows + 16, LANES), F32),
                pltpu.VMEM((2 * blocks * rows, LANES), F32),
                pltpu.VMEM((cols + 2 * LANES, LANES), jnp.bfloat16),
                pltpu.VMEM((4 * groups, cols), jnp.bfloat16),
                pltpu.VMEM((groups, LANES), F32),
                pltpu.VMEM((tall + 16, LANES), F32),
                pltpu.VMEM((8, groups, LANES), F32),
                pltpu.VMEM((2, tall, LANES), F32),
                pltpu.SemaphoreType.DMA((2,)),
                pltpu.SemaphoreType.DMA,
                pltpu.SemaphoreType.DMA,
            ],
            compiler_params=pltpu.CompilerParams(collective_id=0, has_side_effects=True, vmem_limit_bytes=61000000),
        )(tie_order, elevation, data_mask)
        return pl.pallas_call(
            finish,
            out_shape=jax.ShapeDtypeStruct((rows, cols), F32),
            in_specs=[vmem] * len(fields),
            out_specs=pl.BlockSpec(memory_space=pl.ANY),
            scratch_shapes=[pltpu.VMEM((blocks, rows, LANES), F32), pltpu.SemaphoreType.DMA],
            compiler_params=pltpu.CompilerParams(vmem_limit_bytes=40000000),
        )(*given)

    return jax.shard_map(
        on_device, mesh=mesh, in_specs=(P("rows", "cols"), P("rows", "cols"), P()),
        out_specs=P("rows", "cols"), check_vma=False)
```

```python
import functools

import jax
import jax.numpy as jnp
from jax import lax
from jax.experimental import pallas as pl
from jax.experimental.pallas import tpu as pltpu
from jax.sharding import PartitionSpec as P

ITERS = 8
OFFSETS = ((0, 1), (1, 1), (1, 0), (1, -1), (0, -1), (-1, -1), (-1, 0), (-1, 1))
RECIPROCAL = (1.0, 0.7071067811865476) * 4
RETENTION = 0.1
OUTSIDE = 1000.0
LANES = 128
F32 = jnp.float32


def coefficients(tie_ref):
    out = []
    for k in range(8):
        value = jnp.float32(0.0)
        for i in range(8):
            place = jnp.float32((1.0 + 0.5 * (7.0 - i) / 7.0) * RECIPROCAL[k])
            value = jnp.where(tie_ref[i] == k, place, value)
        out.append(value)
    return out


def shift_lanes(before, here, after, step, lane):
    if step == 0:
        return here
    if step < 0:
        return pltpu.roll(jnp.where(lane == LANES - 1, before, here), 1, 1)
    return pltpu.roll(jnp.where(lane == 0, after, here), LANES - 1, 1)


def take_lanes(values, index):
    return jnp.take_along_axis(values, index, axis=1, mode="promise_in_bounds")


def exchange(row_devices, col_devices, tie_hbm, elev_ref, mask_ref, flow_ref, base, inner, outer, inner_edge, outer_edge,
             tie_ref, zp, zl, zr, mask, recip, turned, ones, sums, side, tall, srecv, vrecv, load_sem, tie_sem, recv_sem):
    rows, cols = elev_ref.shape
    groups, blocks = rows // 8, cols // LANES
    crows, halves = groups, groups // 8
    row, col = lax.axis_index("rows"), lax.axis_index("cols")
    far = blocks - 1

    loads = {}
    for j in [0, far] + list(range(1, far)):
        part = pl.ds(j * LANES, LANES)
        loads[j] = (
            pltpu.make_async_copy(elev_ref.at[:, part], zp.at[j, pl.ds(8, rows), :], load_sem.at[0 if j in (0, far) else 1]),
            pltpu.make_async_copy(mask_ref.at[:, part], mask.at[j], load_sem.at[0 if j in (0, far) else 1]))
    barrier = pltpu.get_barrier_semaphore()
    exists = []
    for step_row, step_col in OFFSETS:
        there = jnp.bool_(True)
        if step_row > 0:
            there = row < row_devices - 1
        if step_row < 0:
            there = row > 0
        if step_col > 0:
            there = jnp.logical_and(there, col < col_devices - 1)
        if step_col < 0:
            there = jnp.logical_and(there, col > 0)
        exists.append(there)

    def peer(k):
        return {"rows": row + OFFSETS[k][0], "cols": col + OFFSETS[k][1]}

    for k in (5, 6, 4, 7, 3, 2, 1, 0):
        @pl.when(exists[k])
        def _():
            pl.semaphore_signal(barrier, inc=1, device_id=peer(k), device_id_type=pl.DeviceIdType.MESH)

    for j in loads:
        loads[j][0].start()
        loads[j][1].start()
    tie_load = pltpu.make_async_copy(tie_hbm, tie_ref, tie_sem)
    tie_load.start()

    lane = lax.broadcasted_iota(jnp.int32, (8, LANES), 1)
    sub = lax.broadcasted_iota(jnp.int32, (8, LANES), 0)
    first, last = (lane & 7) == 0, (lane & 7) == 7
    lane_c = lax.broadcasted_iota(jnp.int32, (crows, LANES), 1)
    middle_lanes = jnp.logical_and(lane_c >= LANES // 4, lane_c < 3 * LANES // 4)
    half = LANES // 2
    nothing = jnp.zeros((8, LANES), F32)

    SIDES, UPDOWN = (0, 1, 3, 4, 5, 7), (2, 6)

    taker = lax.broadcasted_iota(jnp.int32, (cols, LANES), 1)
    giver = lax.broadcasted_iota(jnp.int32, (cols, LANES), 0) // 8

    def chosen(here, wanted):
        return (here == wanted).astype(F32).astype(jnp.bfloat16)

    ones[0:cols, :] = chosen(giver, taker)
    for part, start in ((0, 0), (1, far * LANES)):
        ones[cols + part * LANES:cols + (part + 1) * LANES, :] = chosen(giver[start:start + LANES], taker[0:LANES] ^ half)

    order = list(loads)

    def turn(x, step, axis):
        return x if step == 0 else pltpu.roll(x, (-step) % x.shape[axis], axis)

    def row_sums(some):
        for j in some:
            height_sum = jnp.zeros((crows, LANES), F32)
            count_sum = jnp.zeros((crows, LANES), F32)
            for s in range(8):
                valid = mask[j, pl.ds(s, crows, stride=8), :].astype(F32)
                height_sum = height_sum + valid * zp[j, pl.ds(8 + s, crows, stride=8), :]
                count_sum = count_sum + valid
            high = height_sum.astype(jnp.bfloat16)
            rest = height_sum - high.astype(F32)
            middle = rest.astype(jnp.bfloat16)
            low = (rest - middle.astype(F32)).astype(jnp.bfloat16)
            sums[:, j * LANES:(j + 1) * LANES] = jnp.concatenate([count_sum.astype(jnp.bfloat16), high, middle, low], axis=0)
            for number, at in enumerate((8, 9, rows + 6, rows + 7)):
                line = (0, 8, 24 + 2 * crows, 32 + 2 * crows)[number]
                tall[line + j:line + j + 1, :] = zp[j, at:at + 1, :]

    def loaded(number, count):
        whole = turned.at[pl.ds(0, count * rows), :]
        pltpu.make_async_copy(whole, whole, load_sem.at[number]).wait()

    tie_load.wait()
    loaded(0, 4)
    ends = jnp.where(lax.broadcasted_iota(jnp.int32, (rows, LANES), 1) < half, zp[0, 8:8 + rows, :], zp[far, 8:8 + rows, :])
    ends = jnp.transpose(ends)
    tile = jnp.where(sub < 4, pltpu.roll(ends[0:8], 2, 0), pltpu.roll(ends[LANES - 8:LANES], 6, 0))
    tall[16 + 2 * crows:24 + 2 * crows, :] = tile
    parts = [turn(tile, 32 * c - 16, 1) for c in range(4)]

    def packed(at):
        value = nothing
        for c in range(4):
            value = jnp.where(sub == c, pltpu.roll(parts[c], (c - at) % 8, 0), value)
            value = jnp.where(sub == c + 4, pltpu.roll(parts[c], (c + 3 - at) % 8, 0), value)
        return value

    lines = jnp.concatenate([packed(2), packed(4)], axis=0)
    row_sums((0, far))

    def levels(total):
        counts = total[0:crows]
        heights = total[crows:2 * crows] + (total[2 * crows:3 * crows] + total[3 * crows:])
        return heights / (counts + 1.0), counts * (1.0 / 64.0)

    at_ends = jnp.concatenate([sums[:, 0:LANES], sums[:, far * LANES:]], axis=1)
    from_ends = jnp.concatenate([ones[0:LANES, :], ones[far * LANES:cols, :]], axis=0)
    overview, _ = levels(jnp.dot(at_ends, from_ends, preferred_element_type=F32))
    turned_counts = jnp.dot(at_ends[0:crows], ones[cols:, :], preferred_element_type=F32)
    side[...] = jnp.where(
        jnp.logical_and(lane_c >= 16, lane_c < 48), lines, jnp.where(middle_lanes, turned_counts * (1.0 / 64.0), overview))

    pl.semaphore_wait(barrier, functools.reduce(jnp.add, [there.astype(jnp.int32) for there in exists]))

    def copies(k, arriving=False):
        slot = k if arriving else (k + 4) % 8
        if k in UPDOWN:
            src, dst = tall.at[pl.ds(16 if k == 2 else 0, 24 + 2 * crows), :], vrecv.at[slot // 4]
        else:
            src, dst = side, srecv.at[slot]
        return pltpu.make_async_remote_copy(
            src_ref=src, dst_ref=dst, send_sem=tie_sem, recv_sem=recv_sem,
            device_id=peer(k), device_id_type=pl.DeviceIdType.MESH)

    def send(ks):
        for k in ks:
            @pl.when(exists[k])
            def _():
                copies(k).start()

    send((5, 4, 7, 3, 1, 0))

    loaded(1, 2 * blocks - 4)
    row_sums(order[2:])
    overview, runoff = levels(jnp.dot(sums[...], ones[0:cols, :], preferred_element_type=F32))
    tall[16:16 + crows, :] = overview
    tall[16 + crows:16 + 2 * crows, :] = runoff

    send((6, 2))

    for k in range(8):
        @pl.when(jnp.logical_not(exists[k]))
        def _():
            if k in UPDOWN:
                for at in range(0, 24 + 2 * crows, 8):
                    start = 16 + crows if k == 2 else crows
                    vrecv[k // 4, at:at + 8, :] = jnp.full((8, LANES), 0.0 if start <= at < start + crows else OUTSIDE, F32)
            else:
                srecv[k] = jnp.where(jnp.logical_and(lane_c >= 48, lane_c < half + 16), 0.0, OUTSIDE)

    coef = coefficients(tie_ref)

    for ref in (zp, zl, zr, recip):
        for j in range(blocks):
            ref[j, 0:8, :], ref[j, 8 + rows:16 + rows, :] = nothing, nothing

    for g in range(groups):
        at = pl.ds(8 * g + 8, 8)
        for j in range(blocks):
            here = zp[j, at, :]
            before, after = zp[(j - 1) % blocks, at, :], zp[(j + 1) % blocks, at, :]
            zl[j, at, :] = shift_lanes(before, here, after, -1, lane)
            zr[j, at, :] = shift_lanes(before, here, after, 1, lane)
            base[j, pl.ds(8 * g, 8), :] = mask[j, pl.ds(8 * g, 8), :].astype(F32)

    by_column = {-1: zl, 0: zp, 1: zr}

    def within(j, share):
        if j == 0:
            share = jnp.where(lane == 0, 0.0, share)
        if j == far:
            share = jnp.where(lane == LANES - 1, 0.0, share)
        return share

    def leaving(g, j):
        here = zp[j, pl.ds(8 * g + 8, 8), :]
        slopes = {}
        for k, (off_row, off_col) in enumerate(OFFSETS):
            beside = by_column[off_col][j, pl.ds(8 * g + 8 + off_row, 8), :]
            slopes[off_row, off_col] = coef[k] * jnp.maximum(here - beside, 0.0)
        share = within(j, 1.0 / (functools.reduce(jnp.add, slopes.values()) + RETENTION))
        if g == 0:
            share = jnp.where(sub == 0, 0.0, share)
        if g == groups - 1:
            share = jnp.where(sub == 7, 0.0, share)
        recip[j, pl.ds(8 * g + 8, 8), :] = share
        down, up = jnp.where(sub == 7, 0.0, share), jnp.where(sub == 0, 0.0, share)
        out = []
        for c in (-1, 0, 1):
            moved = pltpu.roll(slopes[1, c] * down, 1, 0) + pltpu.roll(slopes[-1, c] * up, 7, 0)
            out.append(moved if c == 0 else moved + slopes[0, c] * share)
        return out

    def across(fields, j):
        west = fields[j - 1][2] if j > 0 else nothing
        east = fields[j + 1][0] if j < far else nothing
        from_west = pltpu.roll(jnp.where(lane == LANES - 1, west, fields[j][2]), 1, 1)
        from_east = pltpu.roll(jnp.where(lane == 0, east, fields[j][0]), LANES - 1, 1)
        kept = fields[j][1] + jnp.where(first, 0.0, from_west) + jnp.where(last, 0.0, from_east)
        return kept, jnp.where(first, from_west, jnp.where(last, from_east, 0.0))

    def settle(g, fields):
        for j in range(blocks):
            at = pl.ds(j * rows + 8 * g, 8)
            inner[at, :], outer[at, :] = across(fields, j)

    for g in range(groups):
        settle(g, [leaving(g, j) for j in range(blocks)])

    def edge_at(number, j, h):
        return pl.ds((number * blocks + j) * groups + 8 * h, 8)

    def compact(number, way, h):
        target = pl.ds(8 + 64 * h + (0 if way == 1 else 7), 8, stride=8)
        source = pl.ds(8 + 64 * h + (-1 if way == 1 else 8), 8, stride=8)
        fields = []
        for j in range(blocks):
            from_z, scale = zp[j, source, :], recip[j, source, :]
            fields.append([
                coef[OFFSETS.index((way, c))] * jnp.maximum(from_z - by_column[c][j, target, :], 0.0) * scale for c in (-1, 0, 1)])
        for j in range(blocks):
            at = edge_at(number, j, h)
            inner_edge[at, :], outer_edge[at, :] = across(fields, j)

    for number, way in enumerate((1, -1)):
        for h in range(halves):
            compact(number, way, h)

    along_rows, along_cols = [
        exists[a].astype(jnp.int32) + exists[b].astype(jnp.int32) for a, b in ((2, 6), (0, 4))]

    def all_of(sem):
        for a in range(min(row_devices - 1, 1), min(row_devices - 1, 2) + 1):
            for b in range(min(col_devices - 1, 1), min(col_devices - 1, 2) + 1):
                lines = crows * (b + a * b) + (24 + 2 * crows) * a
                if lines > 0:
                    @pl.when(jnp.logical_and(along_rows == a, along_cols == b))
                    def _():
                        part = turned.at[pl.ds(0, lines), :]
                        pltpu.make_async_copy(part, part, sem).wait()

    all_of(tie_sem)
    all_of(recv_sem)

    coarse_at = (16, 0)
    tile_at = (16 + 2 * crows, 2 * crows)
    line_at = (0, 24 + 2 * crows - 16)

    def stacked(of_place):
        end = halves - 1
        rows_of = [of_place(None, h) for h in range(halves)] + [of_place(0, 0)]
        return jnp.concatenate(rows_of + [jnp.where(sub < 4, of_place(0, 1), of_place(1, end - 1)), of_place(1, end)], axis=0)

    def middle_of(field):
        def of_place(slot, h):
            if slot is None:
                return tall[16 + field * crows + 8 * h:24 + field * crows + 8 * h, :]
            return vrecv[slot, coarse_at[slot] + field * crows + 8 * h:coarse_at[slot] + field * crows + 8 * h + 8, :]

        return stacked(of_place)

    def beside_of(east):
        ks = {None: 0 if east else 4, 0: 1 if east else 3, 1: 7 if east else 5}
        return stacked(lambda slot, h: srecv[ks[slot], 8 * h:8 * h + 8, :])

    east, west = beside_of(True), beside_of(False)
    nearer = lax.broadcasted_iota(jnp.int32, east.shape, 1) < half
    z = jnp.concatenate([middle_of(0), jnp.where(nearer, east, west)], axis=1)
    supply = jnp.concatenate([middle_of(1), pltpu.roll(jnp.where(nearer, west, east), half, 1)], axis=1)
    beside_z = {step: turn(z, step, 1) for step in (-1, 0, 1)}
    slopes = []
    for k, (step_row, step_col) in enumerate(OFFSETS):
        slopes.append(coef[k] * jnp.maximum(beside_z[0] - turn(beside_z[step_col], step_row, 0), 0.0))
    pairs = [slopes[k] + slopes[k + 4] for k in range(4)]
    share = 1.0 / ((pairs[0] + pairs[1]) + (pairs[2] + (pairs[3] + RETENTION)))

    def core(x):
        return jnp.concatenate([x[0:crows + 8], x[crows + 16:]], axis=0)

    weight = {}
    given = {-1: 0.0, 0: 0.0, 1: 0.0}
    for k, (step_row, step_col) in enumerate(OFFSETS):
        source = slopes[k] * share
        given[step_col] = given[step_col] + turn(source * supply, -step_row, 0)
        weight[step_row, step_col] = source
    flow = core((supply + given[0]) + (turn(given[1], -1, 1) + turn(given[-1], 1, 1)))
    weight = {at: turn(core(weight[at]), -at[1], 1) for at in weight}
    supply = core(supply)

    def sweep(flow):
        moved = {step: turn(flow, -step, 1) for step in (-1, 0, 1)}
        sums = {}
        for step_row in (-1, 0, 1):
            sums[step_row] = functools.reduce(
                jnp.add, [weight[step_row, c] * moved[c] for c in (-1, 0, 1) if (step_row, c) in weight])
        return (supply + sums[0]) + (turn(sums[1], -1, 0) + turn(sums[-1], 1, 0))

    def beside_line(x, step):
        moved = pltpu.roll(x, 1 if step < 0 else LANES - 1, 1)
        edge = pltpu.roll(moved, 1 if step < 0 else 7, 0)
        return jnp.where(lane == (0 if step < 0 else LANES - 1), edge, moved)

    def around(line):
        return {0: line, -1: beside_line(line, -1), 1: beside_line(line, 1)}

    outermost = jnp.logical_or(jnp.logical_and(sub == 0, lane == 0), jnp.logical_and(sub == far, lane == LANES - 1))
    own_lines = ([32 + 2 * crows, 24 + 2 * crows], [0, 8])
    own_lines = [[around(tall[at:at + 8, :]) for at in pair] for pair in own_lines]

    def edge_row(slot):
        inward, number = (-1, 1) if slot == 0 else (1, 0)
        outside = [around(vrecv[slot, line_at[slot] + 8 * i:line_at[slot] + 8 * i + 8, :]) for i in ((0, 1) if slot == 0 else (1, 0))]
        edge, following = own_lines[slot]

        def given(source, near):
            slopes = {at: coef[k] * jnp.maximum(source[0] - near[at[0]][at[1]], 0.0) for k, at in enumerate(OFFSETS)}
            share = jnp.where(outermost, 0.0, 1.0 / (functools.reduce(jnp.add, slopes.values()) + RETENTION))
            return {at: slopes[at] * share for at in slopes}

        def spread(flux, row_step):
            west, east = beside_line(flux[row_step, 1], -1), beside_line(flux[row_step, -1], 1)
            kept = jnp.where(first, 0.0, west) + jnp.where(last, 0.0, east)
            if row_step != 0:
                kept = kept + flux[row_step, 0]
            return kept, jnp.where(first, west, jnp.where(last, east, 0.0))

        from_outside = given(outside[0], {inward: edge, 0: outside[0], -inward: outside[1]})
        from_edge = given(edge, {inward: following, 0: edge, -inward: outside[0]})
        row_at = 0 if slot == 1 else rows - 1
        for values, refs, at in (
                (spread(from_outside, inward), (inner_edge, outer_edge),
                 pl.ds(number * blocks * groups + (0 if slot == 1 else groups - 1), blocks, stride=groups)),
                (spread(from_edge, 0), (inner, outer), pl.ds(row_at, blocks, stride=rows)),
                (spread(from_edge, inward), (inner, outer), pl.ds(row_at + inward, blocks, stride=rows))):
            for value, ref in zip(values, refs):
                ref[at, :] = ref[at, :] + value

    def column(own, left, right):
        beside = jnp.where(sub < 2, pltpu.roll(left, 4, 0), pltpu.roll(right, 4, 0))
        return jnp.where(jnp.logical_and(sub >= 2, sub < 6), own, beside)

    def edge_columns():
        def unpacked(k):
            start = 2 if OFFSETS[k][1] > 0 else 4
            given = srecv[k, 0:8, :] if OFFSETS[k][1] > 0 else srecv[k, 8:16, :]
            value = nothing
            for c in range(4):
                moved = turn(given, 16 - 32 * c, 1)
                pair = jnp.where(sub == start, pltpu.roll(moved, (start - c) % 8, 0), pltpu.roll(moved, (start - 3 - c) % 8, 0))
                value = jnp.where(lane // 32 == c, pair, value)
            return value

        side_tile = {k: unpacked(k) for k in SIDES}
        tall_tile = [vrecv[slot, tile_at[slot]:tile_at[slot] + 8, :] for slot in range(2)]
        tile = tall[16 + 2 * crows:24 + 2 * crows, :]
        below = column(tall_tile[0], side_tile[3], side_tile[1])
        above = column(tall_tile[1], side_tile[5], side_tile[7])
        ze = jnp.concatenate([column(tile, side_tile[4], side_tile[0]), jnp.where(lane < half, below, above)], axis=1)
        sub_e = lax.broadcasted_iota(jnp.int32, (8, 2 * LANES), 0)
        beside_e = {step: turn(ze, step, 1) for step in (-1, 0, 1)}
        flux = {}
        for k, (off_row, off_col) in enumerate(OFFSETS):
            flux[off_row, off_col] = coef[k] * jnp.maximum(ze - turn(beside_e[off_row], off_col, 0), 0.0)
        share_e = 1.0 / (functools.reduce(jnp.add, flux.values()) + RETENTION)

        def lines_of(off_row):
            right, left = flux[off_row, 1] * share_e, flux[off_row, -1] * share_e
            picked = jnp.where(sub_e == 1, right, jnp.where(sub_e == 6, left, 0.0))
            picked = jnp.where(sub_e == 3, pltpu.roll(right, 1, 0), jnp.where(sub_e == 4, pltpu.roll(left, 7, 0), picked))
            if off_row == 0:
                return picked
            return jnp.where(jnp.logical_or(sub_e == 2, sub_e == 5), flux[off_row, 0] * share_e, picked)

        from_above = turn(lines_of(1), -1, 1)[:, :LANES]
        from_below = turn(lines_of(-1), 1, 1)[:, :LANES]
        inside = lines_of(0)[:, :LANES] + jnp.where(first, 0.0, from_above) + jnp.where(last, 0.0, from_below)
        outside = jnp.where(first, from_above, jnp.where(last, from_below, 0.0))
        return inside, outside

    picks = jnp.concatenate([where_lane for where_lane in (
        jnp.where(jnp.logical_or(jnp.logical_and(sub < 4, lane == sub - 2), jnp.logical_and(sub >= 4, lane == sub + (LANES - 6))),
                  jnp.where(jnp.logical_and(sub >= 2, sub < 6), 1.0, 0.0), 0.0),
        jnp.where(jnp.logical_or(jnp.logical_and(sub == 1, lane == 0), jnp.logical_and(sub == 6, lane == LANES - 1)), 1.0, 0.0))], axis=1)
    picks = jnp.concatenate([picks] * 3, axis=0).astype(jnp.bfloat16)

    def upright(lines):
        high = lines.astype(jnp.bfloat16)
        rest = lines - high.astype(F32)
        middle = rest.astype(jnp.bfloat16)
        low = (rest - middle.astype(F32)).astype(jnp.bfloat16)
        split = jnp.concatenate([high.astype(F32), middle.astype(F32), low.astype(F32)], axis=0)
        return jnp.dot(jnp.transpose(split).astype(jnp.bfloat16), picks, preferred_element_type=F32)

    def add_inside(values):
        for field, start in ((inner, 0), (outer, LANES)):
            for g in range(groups):
                value = values[8 * g:8 * g + 8, start:start + LANES]
                for j, chosen in ((0, jnp.where(lane < half, value, 0.0)), (far, jnp.where(lane < half, 0.0, value))):
                    at = pl.ds(j * rows + 8 * g, 8)
                    field[at, :] = field[at, :] + chosen

    def add_outside(values):
        for which, field in enumerate((inner_edge, outer_edge)):
            turned[which * rows:(which + 1) * rows, :] = values[:, which * LANES:(which + 1) * LANES]
            for number in range(2):
                for h in range(halves):
                    value = turned[pl.ds(which * rows + 64 * h + 7 * number, 8, stride=8), :]
                    for j, chosen in ((0, jnp.where(lane < half, value, 0.0)), (far, jnp.where(lane < half, 0.0, value))):
                        at = edge_at(number, j, h)
                        field[at, :] = field[at, :] + chosen

    flow = sweep(flow)
    inside, outside = edge_columns()
    flow = sweep(flow)
    edge_row(0)
    flow = sweep(flow)
    upright_inside, upright_outside = upright(inside), upright(outside)
    flow = sweep(flow)
    edge_row(1)
    flow = sweep(flow)
    flow = sweep(flow)
    add_inside(upright_inside)
    add_outside(upright_outside)
    flow = sweep(flow)

    flow_ref[...] = flow


def finish(flow_ref, base, inner, outer, inner_edge, outer_edge, out_ref, result, sem):
    blocks, rows, _ = base.shape
    groups, far = rows // 8, blocks - 1
    halves = groups // 8
    lane = lax.broadcasted_iota(jnp.int32, (8, LANES), 1)
    sub = lax.broadcasted_iota(jnp.int32, (8, LANES), 0)
    first, last = (lane & 7) == 0, (lane & 7) == 7
    per_block = LANES // 8
    aside = jnp.where(first, -1, jnp.where(last, 1, 0))
    flow = [flow_ref[8 * h:8 * h + 8, :] for h in range(halves + 2)]
    beyond = jnp.where(lax.broadcasted_iota(jnp.int32, (8, 2 * LANES), 0) < 4, flow[halves], flow[halves + 1])
    places = [(x[:, :LANES], x[:, LANES:]) for x in flow[:halves] + [beyond]]
    copies = [
        pltpu.make_async_copy(result.at[j], out_ref.at[:, pl.ds(j * LANES, LANES)], sem) for j in range(blocks)]
    for j in range(blocks):
        index = lane // 8 + j * per_block
        spread = []
        for centre, other in places:
            beside = take_lanes(centre, jnp.clip(index + aside, 0, LANES - 1))
            if j == 0:
                beside = jnp.where(lane == 0, pltpu.roll(other, 1, 1), beside)
            if j == far:
                beside = jnp.where(lane == LANES - 1, pltpu.roll(other, LANES - 1, 1), beside)
            spread.append((take_lanes(centre, index), beside))
        for g in range(groups):
            def level(number):
                return jnp.broadcast_to(spread[g // 8][number][g % 8:g % 8 + 1, :], (8, LANES))

            at, flat = pl.ds(8 * g, 8), pl.ds(j * rows + 8 * g, 8)
            result[j, at, :] = base[j, at, :] + inner[flat, :] * level(0) + outer[flat, :] * level(1)
        for h in range(halves):
            for number in range(2):
                terms = []
                for which in range(2):
                    here = spread[h][which]
                    if number == 0:
                        other = spread[h - 1][which] if h > 0 else spread[-1][which]
                        level = jnp.where(sub == 0, pltpu.roll(other, 1, 0), pltpu.roll(here, 1, 0))
                    else:
                        other = spread[h + 1][which] if h < halves - 1 else spread[-1][which]
                        level = jnp.where(sub == 7, pltpu.roll(other, 7, 0), pltpu.roll(here, 7, 0))
                    flat = pl.ds((number * blocks + j) * groups + 8 * h, 8)
                    terms.append((inner_edge, outer_edge)[which][flat, :] * level)
                at = pl.ds(64 * h + 7 * number, 8, stride=8)
                result[j, at, :] = result[j, at, :] + (terms[0] + terms[1])
        copies[j].start()
    pltpu.make_async_copy(result, result, sem).wait()


def solution(mesh):
    row_devices, col_devices = mesh.shape["rows"], mesh.shape["cols"]

    def on_device(elevation, data_mask, tie_order):
        rows, cols = elevation.shape
        groups, blocks = rows // 8, cols // LANES
        tall = 24 + 2 * groups
        vmem = pl.BlockSpec(memory_space=pltpu.VMEM)
        fields = [
            (2 * groups, 2 * LANES), (blocks, rows, LANES), (blocks * rows, LANES), (blocks * rows, LANES),
            (2 * blocks * groups, LANES), (2 * blocks * groups, LANES)]
        given = pl.pallas_call(
            functools.partial(exchange, row_devices, col_devices),
            out_shape=[pltpu.VMEM(shape, F32) for shape in fields],
            in_specs=[pl.BlockSpec(memory_space=pl.ANY)] * 3,
            out_specs=[vmem] * len(fields),
            scratch_shapes=[
                pltpu.SMEM((8,), jnp.int32),
                pltpu.VMEM((blocks, rows + 16, LANES), F32),
                pltpu.VMEM((blocks, rows + 16, LANES), F32),
                pltpu.VMEM((blocks, rows + 16, LANES), F32),
                pltpu.VMEM((blocks, rows, LANES), jnp.int32),
                pltpu.VMEM((blocks, rows + 16, LANES), F32),
                pltpu.VMEM((2 * blocks * rows, LANES), F32),
                pltpu.VMEM((cols + 2 * LANES, LANES), jnp.bfloat16),
                pltpu.VMEM((4 * groups, cols), jnp.bfloat16),
                pltpu.VMEM((groups, LANES), F32),
                pltpu.VMEM((tall + 16, LANES), F32),
                pltpu.VMEM((8, groups, LANES), F32),
                pltpu.VMEM((2, tall, LANES), F32),
                pltpu.SemaphoreType.DMA((2,)),
                pltpu.SemaphoreType.DMA,
                pltpu.SemaphoreType.DMA,
            ],
            compiler_params=pltpu.CompilerParams(collective_id=0, has_side_effects=True, vmem_limit_bytes=61000000),
        )(tie_order, elevation, data_mask)
        return pl.pallas_call(
            finish,
            out_shape=jax.ShapeDtypeStruct((rows, cols), F32),
            in_specs=[vmem] * len(fields),
            out_specs=pl.BlockSpec(memory_space=pl.ANY),
            scratch_shapes=[pltpu.VMEM((blocks, rows, LANES), F32), pltpu.SemaphoreType.DMA],
            compiler_params=pltpu.CompilerParams(vmem_limit_bytes=40000000),
        )(*given)

    return jax.shard_map(
        on_device, mesh=mesh, in_specs=(P("rows", "cols"), P("rows", "cols"), P()),
        out_specs=P("rows", "cols"), check_vma=False)
```
